64 devices in a mesh: data: 4 (over x, y), model: 16 (over z, core).
Axes of the slice: x: 2, y: 2, z: 8, core: 2. Of those that a mesh axis runs over, the one named last changes fastest.
The devices are a block of a 4x4x8 slice.
Arguments:
- hidden: bfloat16 [128, 5120], P('data'), parts along dimension 0
- w_head: bfloat16 [5120, 131072], P(None, 'model')
- store_keys: bfloat16 [16384, 5120], P('model')
- store_tok: int32 [16384], P('model')
- range_bounds: int32 [16, 17], P('model')
- temperature: float32 [], replicated
- mix_weight: float32 [], replicated
Outputs:
- output: float32 [128, 131072], P('data', 'model'), parts along dimension 0
There are 4 independent parts. The reference program is written for one: setup_inputs(seed, part) draws one part's arguments, and reference() takes and returns one part's arrays. A program takes and returns all parts, laid end to end along the dimension named above; an argument that names none is the same for every part.
All inputs are finite; a program needn't handle non-finite values.
Results may differ from the reference program's by a relative error of at most 0.001.
Values are sent between devices in bfloat16 or wider.
A program may use at most 768 MiB of HBM per device.

```python
import jax
import jax.numpy as jnp
from jax import lax

GROUP_SIZE = 16
BATCH_ROWS = 32
MODEL_DIM = 5120
VOCAB_SIZE = 131072
STORE_LOCAL = 1024


def draw_store_tokens(stream):
    shard_width = VOCAB_SIZE // GROUP_SIZE
    weight_key, first_key, second_key = jax.random.split(stream, 3)
    shard_ids = jnp.arange(GROUP_SIZE, dtype=jnp.int32)
    zipf_weight = (4 * GROUP_SIZE) // (shard_ids + 4)
    weights = jax.random.randint(weight_key, (GROUP_SIZE, GROUP_SIZE), 1, 5, jnp.int32) * zipf_weight[None, :]
    cum_weight = jnp.concatenate([jnp.zeros((GROUP_SIZE, 1), jnp.int32), jnp.cumsum(weights, axis=1)], axis=1)
    range_bounds = (STORE_LOCAL * cum_weight) // cum_weight[:, GROUP_SIZE:]
    positions = jnp.arange(STORE_LOCAL, dtype=jnp.int32)
    owner_shard = jax.vmap(lambda bound_row: jnp.searchsorted(bound_row[1:GROUP_SIZE], positions, side='right'))(range_bounds)
    column = jnp.minimum(
        jax.random.randint(first_key, (GROUP_SIZE, STORE_LOCAL), 0, shard_width, jnp.int32),
        jax.random.randint(second_key, (GROUP_SIZE, STORE_LOCAL), 0, shard_width, jnp.int32))
    store_tok = jnp.sort(owner_shard.astype(jnp.int32) * shard_width + column, axis=1)
    return store_tok.reshape(GROUP_SIZE * STORE_LOCAL).astype(jnp.int32), range_bounds.astype(jnp.int32)


def setup_inputs(seed: int = 0, part: int = 0) -> dict:
    root_key = jax.random.key(seed)
    streams = jax.random.split(root_key, 7)
    hidden = jax.random.normal(jax.random.fold_in(streams[0], part), (BATCH_ROWS, MODEL_DIM), jnp.float32)
    head_scale = 2.5 * MODEL_DIM ** -0.5

    def draw_head_rows(row_stream):
        draw = jax.random.normal(row_stream, (128, VOCAB_SIZE), jnp.float32)
        return (draw * head_scale).astype(jnp.bfloat16)

    w_head = lax.map(draw_head_rows, jax.random.split(streams[1], MODEL_DIM // 128)).reshape(MODEL_DIM, VOCAB_SIZE)
    spread = jax.random.uniform(streams[2], (GROUP_SIZE,), jnp.float32, -1.0, 1.0)
    key_scale = jnp.sqrt(1.0 + 2.5 * spread * MODEL_DIM ** -0.5)

    def draw_shard(stream_and_scale):
        shard_stream, shard_scale = stream_and_scale
        draw = jax.random.normal(shard_stream, (STORE_LOCAL, MODEL_DIM), jnp.float32)
        return (draw * shard_scale).astype(jnp.bfloat16)

    store_keys = lax.map(draw_shard, (jax.random.split(streams[3], GROUP_SIZE), key_scale))
    store_keys = store_keys.reshape(GROUP_SIZE * STORE_LOCAL, MODEL_DIM)
    store_tok, range_bounds = draw_store_tokens(streams[4])
    temperature = jax.random.uniform(streams[5], (), jnp.float32, 2.0, 3.0) * MODEL_DIM ** 0.5
    mix_weight = jax.random.uniform(streams[6], (), jnp.float32, 0.2, 0.7)
    return {'hidden': hidden.astype(jnp.bfloat16), 'w_head': w_head, 'store_keys': store_keys,
            'store_tok': store_tok, 'range_bounds': range_bounds,
            'temperature': temperature, 'mix_weight': mix_weight}


def reference(hidden, w_head, store_keys, store_tok, range_bounds, temperature, mix_weight):
    shard_width = VOCAB_SIZE // GROUP_SIZE
    keys_shards = store_keys.reshape(GROUP_SIZE, STORE_LOCAL, MODEL_DIM)

    def shard_scores(keys_local):
        keys_wide = keys_local.astype(jnp.float32)
        key_norm = jnp.sum(keys_wide * keys_wide, axis=1)
        cross_dot = jnp.dot(keys_local, hidden.T, preferred_element_type=jnp.float32)
        return (2.0 * cross_dot - key_norm[:, None]) / temperature

    scores = lax.map(shard_scores, keys_shards).reshape(GROUP_SIZE * STORE_LOCAL, BATCH_ROWS)
    row_max = jnp.max(scores, axis=0)
    kernel = jnp.exp(scores - row_max[None, :])
    knn_total = jnp.sum(kernel, axis=0)
    tok_grid = store_tok.reshape(GROUP_SIZE, STORE_LOCAL)
    owner = tok_grid // shard_width
    range_lo = jnp.take_along_axis(range_bounds, owner, axis=1)
    range_hi = jnp.take_along_axis(range_bounds, owner + 1, axis=1)
    positions = jnp.arange(STORE_LOCAL)[None, :]
    counted = (positions >= range_lo) & (positions < range_hi)
    segment = jnp.where(counted, tok_grid, VOCAB_SIZE).reshape(GROUP_SIZE * STORE_LOCAL)
    hist_full = jax.ops.segment_sum(kernel, segment, num_segments=VOCAB_SIZE + 1)[:VOCAB_SIZE]
    knn_prob = hist_full.T / knn_total[:, None]
    logits = jnp.dot(hidden, w_head, preferred_element_type=jnp.float32)
    lm_max = jnp.max(logits, axis=1, keepdims=True)
    lm_exp = jnp.exp(logits - lm_max)
    lm_prob = lm_exp / jnp.sum(lm_exp, axis=1, keepdims=True)
    return jnp.log(mix_weight * knn_prob + (1.0 - mix_weight) * lm_prob)
```

```python
import functools

import jax
import jax.numpy as jnp
from jax import lax
from jax.experimental import pallas as pl
from jax.experimental.pallas import tpu as pltpu
from jax.sharding import PartitionSpec as P

MESH_ID = pl.DeviceIdType.MESH
LANES = 128
BLOCK = 256
SLOTS = 16
F32 = jnp.float32


def lane_groups(x, op):
    x = op(x, pltpu.roll(x, 64, 1))
    return op(x, pltpu.roll(x, 32, 1))


def score_kernel(group, hid_ref, tok_ref, rb_ref, tau_ref, lam_ref, keys_ref, w_ref,
                 ec_out, logit_out, meta_out, stat_out,
                 kbuf, wbuf, gath, ecs, meta, logits, mrun, srun, stats,
                 ksem, wsem, osem, rs, rr, ls, lr, ps, pr, ms, mr, ss, sr):
    me = lax.axis_index('model')
    chips = group // 2
    chip, core = me // 2, me % 2
    partner = me + 1 - 2 * core
    right = ((chip + 1) % chips) * 2 + core
    left = ((chip + chips - 1) % chips) * 2 + core
    rows, dim = hid_ref.shape
    quarter = kbuf.shape[1]
    half = quarter // 2
    blocks = logits.shape[1] // BLOCK
    far = chips // 2

    barrier = pltpu.get_barrier_semaphore()
    for p in range(1, group):
        pl.semaphore_signal(barrier, inc=1, device_id={'model': (me + p) % group}, device_id_type=MESH_ID)

    def key_copy(c):
        return pltpu.make_async_copy(keys_ref.at[pl.ds(pl.multiple_of(c * quarter, quarter), quarter)],
                                     kbuf.at[c], ksem.at[c])

    def w_copy(i):
        slot = lax.rem(i, SLOTS)
        return pltpu.make_async_copy(w_ref.at[:, pl.ds(pl.multiple_of(i * BLOCK, BLOCK), BLOCK)],
                                     wbuf.at[slot], wsem.at[slot])

    for c in range(4):
        key_copy(c).start()
    for i in range(SLOTS):
        w_copy(i).start()

    meta[me] = jnp.zeros(meta.shape[1:], jnp.int32)
    meta[me, 0:8, :] = tok_ref[...]
    meta[me, 8:9, 0:rb_ref.shape[1]] = rb_ref[...]
    mrun[...] = jnp.full(mrun.shape, -3.0e38, F32)
    srun[...] = jnp.zeros(srun.shape, F32)

    lane = lax.broadcasted_iota(jnp.int32, (quarter, LANES), 1)

    def score_step(c, carry):
        key_copy(c).wait()
        norm = jnp.zeros((quarter, LANES), F32)
        for t in range(dim // LANES):
            x = kbuf[c, :, t * LANES:(t + 1) * LANES].astype(F32)
            norm = norm + x * x
        norm = jnp.sum(norm, axis=1, keepdims=True)
        hid4 = jnp.concatenate([hid_ref[...]] * 4, axis=0)
        dot = lax.dot_general(kbuf[c], hid4, (((1,), (1,)), ((), ())), preferred_element_type=F32)
        score = (2.0 * dot - norm) / tau_ref[0]
        gath[me] = jnp.where(lane // rows == c, score, gath[me])
        return carry

    gath[me] = jnp.zeros(gath.shape[1:], F32)
    lax.fori_loop(0, 4, score_step, 0)

    pl.semaphore_wait(barrier, group - 1)

    def remote(ref, slot, part, send, recv, target):
        view = ref.at[slot] if part is None else ref.at[slot, pl.ds(part * half, half)]
        return pltpu.make_async_remote_copy(view, view, send, recv, device_id={'model': target},
                                            device_id_type=MESH_ID)

    def origin(step, sign):
        return ((chip + chips + sign * step) % chips) * 2 + core

    def right_piece(s, h):
        return remote(gath, origin(s - 1, -1), h, rs.at[2 * s - 2 + h], rr.at[2 * s - 2 + h], right)

    def right_landed(s, h):
        return remote(gath, origin(s, -1), h, rs.at[2 * s - 2 + h], rr.at[2 * s - 2 + h], right)

    def left_piece(s, h):
        return remote(gath, origin(s - 1, 1), h, ls.at[2 * s - 2 + h], lr.at[2 * s - 2 + h], left)

    def left_landed(s, h):
        return remote(gath, origin(s, 1), h, ls.at[2 * s - 2 + h], lr.at[2 * s - 2 + h], left)

    def across(step, h, q):
        return remote(gath, origin(step, -1), h, ps.at[q, h], pr.at[q, h], partner)

    def across_landed(step, h, q):
        slot = origin(step, -1) + 1 - 2 * core
        return remote(gath, slot, h, ps.at[q, h], pr.at[q, h], partner)

    for h in range(2):
        right_piece(1, h).start()
        left_piece(1, h).start()
    for h in range(2):
        across(0, h, 0).start()

    def meta_copy(p, slot):
        return remote(meta, slot, None, ms.at[p], mr.at[p], (me + p) % group)

    for p in range(1, group):
        meta_copy(p, me).start()

    right_order = [(s, h) for s in range(1, far) for h in range(2)] + [(far, 0)]
    left_order = [(s, h) for s in range(1, far) for h in range(2)] + [(far, 1)]

    def ring_event(e):
        s, h = right_order[e]
        right_landed(s, h).wait_recv()
        if (s + 1, h) in right_order:
            right_piece(s + 1, h).start()
        across(s, h, s).start()
        s, h = left_order[e]
        left_landed(s, h).wait_recv()
        if (s + 1, h) in left_order:
            left_piece(s + 1, h).start()
        across(chips - s, h, chips - s).start()

    def normalise():
        for q in range(chips):
            for h in range(2):
                across_landed(q, h, q).wait_recv()

        def max_step(g, acc):
            return jnp.maximum(acc, jnp.max(gath[g].reshape(quarter // 8, 8, LANES), axis=0))

        top = lax.fori_loop(0, group, max_step, jnp.full((8, LANES), -3.0e38, F32))
        top = lane_groups(jnp.broadcast_to(jnp.max(top, axis=0, keepdims=True), (8, LANES)), jnp.maximum)[0:1]

        def exp_step(g, acc):
            e = jnp.exp(gath[g] - top)
            ecs[g] = e
            return acc + jnp.sum(e.reshape(quarter // 8, 8, LANES), axis=0)

        total = lax.fori_loop(0, group, exp_step, jnp.zeros((8, LANES), F32))
        total = lane_groups(jnp.broadcast_to(jnp.sum(total, axis=0, keepdims=True), (8, LANES)), jnp.add)[0:1]
        scale = lam_ref[0] / total

        def scale_step(g, carry):
            ecs[g] = ecs[g] * scale
            return carry

        lax.fori_loop(0, group, scale_step, 0)

    ec_copy = pltpu.make_async_copy(ecs, ec_out, osem.at[0])
    logit_copy = pltpu.make_async_copy(logits, logit_out, osem.at[1])
    meta_back = pltpu.make_async_copy(meta, meta_out, osem.at[2])

    def w_step(i, carry):
        slot = lax.rem(i, SLOTS)
        w_copy(i).wait()
        acc = jnp.dot(hid_ref[...], wbuf[slot], preferred_element_type=F32)
        logits[:, pl.ds(pl.multiple_of(i * BLOCK, BLOCK), BLOCK)] = acc

        @pl.when(i + SLOTS < blocks)
        def _():
            w_copy(i + SLOTS).start()

        parts = [acc[:, t * LANES:(t + 1) * LANES] for t in range(BLOCK // LANES)]
        old = mrun[...]
        new = functools.reduce(jnp.maximum, parts, old)
        srun[...] = sum((jnp.exp(x - new) for x in parts), srun[...] * jnp.exp(old - new))
        mrun[...] = new

        for e in range(len(right_order)):
            pl.when(i == 4 + 2 * e)(functools.partial(ring_event, e))

        @pl.when(i == 6 + 2 * len(right_order))
        def _():
            normalise()
            ec_copy.start()
        return carry

    lax.fori_loop(0, blocks, w_step, 0)

    peak = jnp.max(mrun[...], axis=1, keepdims=True)
    tot = jnp.sum(srun[...] * jnp.exp(mrun[...] - peak), axis=1, keepdims=True)
    peak = jnp.broadcast_to(peak, (rows, LANES))
    tot = jnp.broadcast_to(tot, (rows, LANES))
    tile_lane = lax.broadcasted_iota(jnp.int32, (8, LANES), 1)
    tile = jnp.zeros((8, LANES), F32)
    for v in range(rows // 8):
        tile = jnp.where(tile_lane == v, peak[8 * v:8 * v + 8], tile)
        tile = jnp.where(tile_lane == 64 + v, tot[8 * v:8 * v + 8], tile)
    stats[me] = tile

    def stat_copy(p, slot):
        return remote(stats, slot, None, ss.at[p], sr.at[p], (me + p) % group)

    for p in range(1, group):
        stat_copy(p, me).start()
    logit_copy.start()
    for p in range(1, group):
        meta_copy(p, (me + group - p) % group).wait_recv()
    meta_back.start()
    for p in range(1, group):
        stat_copy(p, (me + group - p) % group).wait_recv()

    high = stats[0]
    for g in range(1, group):
        high = jnp.maximum(high, stats[g])
    total = jnp.zeros((8, LANES), F32)
    for g in range(group):
        one = stats[g]
        total = total + pltpu.roll(one, 64, 1) * jnp.exp(jnp.where(tile_lane < 8, one - high, 0.0))
    stat_out[0:8] = high
    stat_out[8:16] = (1.0 - lam_ref[0]) / jnp.where(tile_lane < rows // 8, total, 1.0)

    for s, h in right_order:
        right_piece(s, h).wait_send()
    for s, h in left_order:
        left_piece(s, h).wait_send()
    for q in range(chips):
        for h in range(2):
            across(q, h, q).wait_send()
    for p in range(1, group):
        meta_copy(p, me).wait_send()
        stat_copy(p, me).wait_send()
    ec_copy.wait()
    logit_copy.wait()
    meta_back.wait()


def mix_kernel(group, meta_hbm, ec_hbm, logit_hbm, stat_ref, out_ref, meta, ec, logits, hist, sems):
    me = lax.axis_index('model')
    rows, width = logits.shape
    quarter = ec.shape[1]
    copies = [pltpu.make_async_copy(a, b, sems.at[i])
              for i, (a, b) in enumerate(((meta_hbm, meta), (ec_hbm, ec), (logit_hbm, logits)))]
    for c in copies:
        c.start()

    def zero_step(i, carry):
        hist[pl.ds(pl.multiple_of(i * LANES, LANES), LANES), :] = jnp.zeros((LANES, LANES), F32)
        return carry

    lax.fori_loop(0, width // LANES, zero_step, 0)
    copies[0].wait()
    copies[1].wait()
    lane = lax.broadcasted_iota(jnp.int32, (1, LANES), 1)
    base = me * width

    def source_step(g, carry):
        low, high = meta[g, 8, me], meta[g, 8, me + 1]
        for k in range(4):
            mask = lane // rows == k

            def entry_step(i, c):
                t = meta[g, lax.shift_right_logical(i, 7), jnp.bitwise_and(i, LANES - 1)] - base
                row = ec[g, pl.ds(i - k * quarter, 1), :]
                hist[pl.ds(t, 1), :] = hist[pl.ds(t, 1), :] + jnp.where(mask, row, 0.0)
                return c

            lax.fori_loop(jnp.maximum(low, k * quarter), jnp.minimum(high, (k + 1) * quarter), entry_step, 0)
        return carry

    lax.fori_loop(0, group, source_step, 0)
    copies[2].wait()
    peak = jnp.concatenate([stat_ref[0:8, v:v + 1] for v in range(rows // 8)], axis=0)
    share = jnp.concatenate([stat_ref[8:16, v:v + 1] for v in range(rows // 8)], axis=0)

    def out_step(i, carry):
        for u in range(4):
            at = pl.ds(pl.multiple_of((i * 4 + u) * LANES, LANES), LANES)
            turned = hist[at, :].T
            knn = turned[0:rows]
            for k in range(1, 4):
                knn = knn + turned[k * rows:(k + 1) * rows]
            out_ref[:, at] = jnp.log(knn + jnp.exp(logits[:, at] - peak) * share)
        return carry

    lax.fori_loop(0, width // LANES // 4, out_step, 0)


def solution(mesh):
    group = mesh.shape['model']

    def local_step(hidden, w_local, keys_local, tok_local, bounds_local, temperature, mix_weight):
        rows, dim = hidden.shape
        width = w_local.shape[1]
        store = keys_local.shape[0]
        quarter = store // 4
        chips = group // 2
        vmem = pl.BlockSpec(memory_space=pltpu.VMEM)
        smem = pl.BlockSpec(memory_space=pltpu.SMEM)
        hbm = pl.BlockSpec(memory_space=pltpu.HBM)
        dma = pltpu.SemaphoreType.DMA
        gathered = (group, quarter, LANES)
        meta_shape = (group, 16, LANES)
        pieces = chips - 1
        ec, logits, meta, stat = pl.pallas_call(
            functools.partial(score_kernel, group),
            out_shape=(jax.ShapeDtypeStruct(gathered, F32), jax.ShapeDtypeStruct((rows, width), F32),
                       jax.ShapeDtypeStruct(meta_shape, jnp.int32), jax.ShapeDtypeStruct((16, LANES), F32)),
            in_specs=[vmem, vmem, vmem, smem, smem, hbm, hbm],
            out_specs=(hbm, hbm, hbm, vmem),
            scratch_shapes=[
                pltpu.VMEM((4, quarter, dim), jnp.bfloat16),
                pltpu.VMEM((SLOTS, dim, BLOCK), jnp.bfloat16),
                pltpu.VMEM(gathered, F32),
                pltpu.VMEM(gathered, F32),
                pltpu.VMEM(meta_shape, jnp.int32),
                pltpu.VMEM((rows, width), F32),
                pltpu.VMEM((rows, LANES), F32),
                pltpu.VMEM((rows, LANES), F32),
                pltpu.VMEM((group, 8, LANES), F32),
                dma((4,)), dma((SLOTS,)), dma((3,)),
                dma((pieces + 1,)), dma((pieces + 1,)), dma((pieces + 1,)), dma((pieces + 1,)),
                dma((chips, 2)), dma((chips, 2)),
                dma((group,)), dma((group,)), dma((group,)), dma((group,)),
            ],
            compiler_params=pltpu.CompilerParams(collective_id=0, has_side_effects=True,
                                                 vmem_limit_bytes=64 * 1024 * 1024 - 65536),
            name='score_gather_head',
        )(hidden, tok_local.reshape(store // LANES, LANES), bounds_local, temperature.reshape(1),
          mix_weight.reshape(1), keys_local, w_local)
        return pl.pallas_call(
            functools.partial(mix_kernel, group),
            out_shape=jax.ShapeDtypeStruct((rows, width), F32),
            in_specs=[hbm, hbm, hbm, vmem],
            out_specs=vmem,
            scratch_shapes=[
                pltpu.SMEM(meta_shape, jnp.int32),
                pltpu.VMEM(gathered, F32),
                pltpu.VMEM((rows, width), F32),
                pltpu.VMEM((width, LANES), F32),
                dma((3,)),
            ],
            compiler_params=pltpu.CompilerParams(vmem_limit_bytes=64 * 1024 * 1024 - 65536),
            name='bin_mix',
        )(meta, ec, logits, stat)

    return jax.shard_map(local_step, mesh=mesh,
                         in_specs=(P('data', None), P(None, 'model'), P('model', None), P('model'),
                                   P('model', None), P(), P()),
                         out_specs=P('data', 'model'), check_vma=False)
```

```python
import functools

import jax
import jax.numpy as jnp
from jax import lax
from jax.experimental import pallas as pl
from jax.experimental.pallas import tpu as pltpu
from jax.sharding import PartitionSpec as P

MESH_ID = pl.DeviceIdType.MESH
LANES = 128
BLOCK = 256
SLOTS = 16
F32 = jnp.float32
LOWEST = float(jnp.finfo(jnp.float32).min)
VMEM_BYTES = 64 * 1024 * 1024 - 65536
EXTRA = 16


def lane_groups(x, op):
    x = op(x, pltpu.roll(x, 64, 1))
    return op(x, pltpu.roll(x, 32, 1))


def score_kernel(group, hid_ref, tok_ref, rb_ref, tau_ref, lam_ref, keys_ref, w_ref,
                 gath_out, logit_out, meta_out, scale_out, stat_out,
                 kbuf, wbuf, gath, toks, meta, logits, mrun, srun, stats,
                 ksem, wsem, osem, rs, rr, ls, lr, ps, pr, ss, sr):
    me = lax.axis_index('model')
    chips = group // 2
    chip, core = me // 2, me % 2
    partner = me + 1 - 2 * core
    right = ((chip + 1) % chips) * 2 + core
    left = ((chip + chips - 1) % chips) * 2 + core
    rows, dim = hid_ref.shape
    quarter = kbuf.shape[1]
    half = (quarter + EXTRA) // 2
    width = logits.shape[1]
    blocks = width // BLOCK
    far = chips // 2
    extra = quarter + 8

    barrier = pltpu.get_barrier_semaphore()
    for p in range(1, group):
        pl.semaphore_signal(barrier, inc=1, device_id={'model': (me + p) % group}, device_id_type=MESH_ID)

    def key_copy(c):
        return pltpu.make_async_copy(keys_ref.at[pl.ds(pl.multiple_of(c * quarter, quarter), quarter)],
                                     kbuf.at[c], ksem.at[c])

    def w_copy(i):
        slot = lax.rem(i, SLOTS)
        return pltpu.make_async_copy(w_ref.at[:, pl.ds(pl.multiple_of(i * BLOCK, BLOCK), BLOCK)],
                                     wbuf.at[slot], wsem.at[slot])

    for c in range(4):
        key_copy(c).start()
    for i in range(SLOTS):
        w_copy(i).start()

    mrun[...] = jnp.full(mrun.shape, LOWEST, F32)
    srun[...] = jnp.zeros(srun.shape, F32)
    tok = tok_ref[...].astype(F32)
    gath[me, pl.ds(quarter, 8), :] = tok
    gath[me, pl.ds(extra, 8), :] = jnp.zeros((8, LANES), F32)
    gath[me, pl.ds(extra, 1), 0:rb_ref.shape[1]] = rb_ref[...].astype(F32)
    for h in range(2):
        toks[h * LANES:(h + 1) * LANES, :] = jnp.concatenate(
            [jnp.broadcast_to(tok[2 * k + h:2 * k + h + 1], (rows, LANES)) for k in range(4)], axis=0).T

    lane = lax.broadcasted_iota(jnp.int32, (quarter, LANES), 1)
    gath[me, 0:quarter, :] = jnp.zeros((quarter, LANES), F32)

    def score_step(c, carry):
        key_copy(c).wait()
        norm = jnp.zeros((quarter, LANES), F32)
        for t in range(dim // LANES):
            x = kbuf[c, :, t * LANES:(t + 1) * LANES].astype(F32)
            norm = norm + x * x
        norm = jnp.sum(norm, axis=1, keepdims=True)
        hid4 = jnp.concatenate([hid_ref[...]] * 4, axis=0)
        dot = lax.dot_general(kbuf[c], hid4, (((1,), (1,)), ((), ())), preferred_element_type=F32)
        score = (2.0 * dot - norm) / tau_ref[0]
        score = jnp.where(lane // rows == c, score, gath[me, 0:quarter, :])
        gath[me, 0:quarter, :] = score
        return carry

    lax.fori_loop(0, 4, score_step, 0)

    top = functools.reduce(jnp.maximum, [gath[me, r * 8:r * 8 + 8, :] for r in range(quarter // 8)])
    top = lane_groups(jnp.broadcast_to(jnp.max(top, axis=0, keepdims=True), (8, LANES)), jnp.maximum)
    sub = lax.broadcasted_iota(jnp.int32, (8, LANES), 0)

    def exp_step(r, total):
        at = pl.ds(pl.multiple_of(r * 8, 8), 8)
        e = jnp.exp(gath[me, at, :] - top)
        total = total + e
        ids = toks[at, :]
        last = (ids != pltpu.roll(ids, 7, 0)) | (sub == 7)
        for d in (1, 2, 4):
            same = (ids == pltpu.roll(ids, d, 0)) & (sub >= d)
            e = e + jnp.where(same, pltpu.roll(e, d, 0), 0.0)
        gath[me, at, :] = jnp.where(last, e, 0.0)
        return total

    total = lax.fori_loop(0, quarter // 8, exp_step, jnp.zeros((8, LANES), F32), unroll=8)
    total = lane_groups(jnp.broadcast_to(jnp.sum(total, axis=0, keepdims=True), (8, LANES)), jnp.add)
    gath[me, pl.ds(extra + 1, 1), :] = top[0:1]
    gath[me, pl.ds(extra + 2, 1), :] = total[0:1]

    pl.semaphore_wait(barrier, group - 1)

    def remote(ref, slot, part, send, recv, target):
        view = ref.at[slot] if part is None else ref.at[slot, pl.ds(part * half, half)]
        return pltpu.make_async_remote_copy(view, view, send, recv, device_id={'model': target},
                                            device_id_type=MESH_ID)

    def origin(step, sign):
        return ((chip + chips + sign * step) % chips) * 2 + core

    def right_piece(s, h):
        return remote(gath, origin(s - 1, -1), h, rs.at[2 * s - 2 + h], rr.at[2 * s - 2 + h], right)

    def right_landed(s, h):
        return remote(gath, origin(s, -1), h, rs.at[2 * s - 2 + h], rr.at[2 * s - 2 + h], right)

    def left_piece(s, h):
        return remote(gath, origin(s - 1, 1), h, ls.at[2 * s - 2 + h], lr.at[2 * s - 2 + h], left)

    def left_landed(s, h):
        return remote(gath, origin(s, 1), h, ls.at[2 * s - 2 + h], lr.at[2 * s - 2 + h], left)

    def across(step, h, q):
        return remote(gath, origin(step, -1), h, ps.at[q, h], pr.at[q, h], partner)

    def across_landed(step, h, q):
        slot = origin(step, -1) + 1 - 2 * core
        return remote(gath, slot, h, ps.at[q, h], pr.at[q, h], partner)

    for h in range(2):
        right_piece(1, h).start()
        left_piece(1, h).start()
    for h in range(2):
        across(0, h, 0).start()

    right_order = [(s, h) for s in range(1, far) for h in range(2)] + [(far, 0)]
    left_order = [(s, h) for s in range(1, far) for h in range(2)] + [(far, 1)]

    def ring_event(e):
        s, h = right_order[e]
        right_landed(s, h).wait_recv()
        if (s + 1, h) in right_order:
            right_piece(s + 1, h).start()
        across(s, h, s).start()
        s, h = left_order[e]
        left_landed(s, h).wait_recv()
        if (s + 1, h) in left_order:
            left_piece(s + 1, h).start()
        across(chips - s, h, chips - s).start()

    gath_copy = pltpu.make_async_copy(gath, gath_out, osem.at[0])
    meta_copy = pltpu.make_async_copy(meta, meta_out, osem.at[1])

    def gathered():
        for q in range(chips):
            for h in range(2):
                across_landed(q, h, q).wait_recv()
        gath_copy.start()
        tile_lane = lax.broadcasted_iota(jnp.int32, (8, LANES), 1)
        place = lax.broadcasted_iota(jnp.int32, (8, LANES), 0) * LANES + tile_lane
        high = functools.reduce(jnp.maximum, [gath[g, extra + 1:extra + 2, :] for g in range(group)])
        shares = [jnp.exp(gath[g, extra + 1:extra + 2, :] - high) for g in range(group)]
        whole = sum(gath[g, extra + 2:extra + 3, :] * shares[g] for g in range(group))
        for g in range(group):
            scale_out[g:g + 1, :] = shares[g] * (lam_ref[0] / whole)

        def index_step(g, carry):
            bounds = gath[g, extra:extra + 8, :]
            first = jnp.sum(jnp.where(tile_lane == me, bounds, 0.0), axis=1, keepdims=True)[0:1].astype(jnp.int32)
            after = jnp.sum(jnp.where(tile_lane == me + 1, bounds, 0.0), axis=1, keepdims=True)[0:1].astype(jnp.int32)
            ids = gath[g, quarter:quarter + 8, :].astype(jnp.int32)
            meta[g, 0:8, :] = jnp.where((place >= first) & (place < after), ids - me * width, width)
            meta[g, 8:16, :] = bounds.astype(jnp.int32)
            return carry

        lax.fori_loop(0, group, index_step, 0, unroll=4)
        meta_copy.start()

    def block_stats(i, keep):
        parts = [logits[:, pl.ds(pl.multiple_of(i * BLOCK, BLOCK) + t * LANES, LANES)] for t in range(BLOCK // LANES)]
        old = mrun[...]
        new = functools.reduce(jnp.maximum, parts, old)
        srun[...] = sum((jnp.exp(x - new) for x in parts), srun[...] * jnp.exp(old - new)) * keep
        mrun[...] = new

    bands = 4
    band = width // bands

    def logit_copy(b):
        at = pl.ds(b * band, band)
        return pltpu.make_async_copy(logits.at[:, at], logit_out.at[:, at], osem.at[2 + b])

    logits[:, 0:BLOCK] = jnp.full((rows, BLOCK), LOWEST, F32)

    def w_step(i, carry):
        slot = lax.rem(i, SLOTS)
        w_copy(i).wait()
        block_stats(jnp.maximum(i - 1, 0), jnp.where(i > 0, 1.0, 0.0))
        acc = jnp.dot(hid_ref[...], wbuf[slot], preferred_element_type=F32)
        logits[:, pl.ds(pl.multiple_of(i * BLOCK, BLOCK), BLOCK)] = acc

        @pl.when(i + SLOTS < blocks)
        def _():
            w_copy(i + SLOTS).start()

        for e in range(len(right_order)):
            pl.when(i == 4 + 2 * e)(functools.partial(ring_event, e))
        pl.when(i == 6 + 2 * len(right_order))(gathered)
        for b in range(bands - 1):
            pl.when(i == (b + 1) * (blocks // bands))(logit_copy(b).start)
        return carry

    lax.fori_loop(0, blocks, w_step, 0)
    block_stats(blocks - 1, 1.0)
    logit_copy(bands - 1).start()

    peak = jnp.max(mrun[...], axis=1, keepdims=True)
    tot = jnp.sum(srun[...] * jnp.exp(mrun[...] - peak), axis=1, keepdims=True)
    pad = jnp.zeros((64 - rows, LANES), F32)
    square = jnp.concatenate([jnp.broadcast_to(peak, (rows, LANES)), pad, jnp.broadcast_to(tot, (rows, LANES)), pad],
                             axis=0)
    stats[me] = square.T[0:1]

    def stat_copy(p, slot):
        return remote(stats, slot, None, ss.at[p], sr.at[p], (me + p) % group)

    for p in range(1, group):
        stat_copy(p, me).start()
    for p in range(1, group):
        stat_copy(p, (me + group - p) % group).wait_recv()

    row_lane = lax.broadcasted_iota(jnp.int32, (1, LANES), 1)
    every = [stats[g] for g in range(group)]
    high = functools.reduce(jnp.maximum, every)
    total = jnp.zeros((1, LANES), F32)
    for one in every:
        moved = pltpu.roll(jnp.broadcast_to(one, (8, LANES)), 64, 1)[0:1]
        total = total + moved * jnp.exp(jnp.where(row_lane < rows, one - high, 0.0))
    share = (1.0 - lam_ref[0]) / jnp.where(row_lane < rows, total, 1.0)
    stat_out[0:rows] = jnp.broadcast_to(high, (LANES, LANES)).T[0:rows]
    stat_out[rows:2 * rows] = jnp.broadcast_to(share, (LANES, LANES)).T[0:rows]

    for s, h in right_order:
        right_piece(s, h).wait_send()
    for s, h in left_order:
        left_piece(s, h).wait_send()
    for q in range(chips):
        for h in range(2):
            across(q, h, q).wait_send()
    for p in range(1, group):
        stat_copy(p, me).wait_send()
    gath_copy.wait()
    meta_copy.wait()
    for b in range(bands):
        logit_copy(b).wait()


def mix_kernel(group, meta_hbm, gath_hbm, logit_hbm, scale_ref, stat_ref, out_ref, meta, gath, logits, hist, sems):
    me = lax.axis_index('model')
    rows, width = logits.shape
    copies = [pltpu.make_async_copy(a, b, sems.at[i])
              for i, (a, b) in enumerate(((meta_hbm, meta), (gath_hbm, gath), (logit_hbm, logits)))]
    for c in copies:
        c.start()

    def zero_step(i, carry):
        hist[pl.ds(pl.multiple_of(i * LANES, LANES), LANES), :] = jnp.zeros((LANES, LANES), F32)
        return carry

    lax.fori_loop(0, width // LANES, zero_step, 0)
    hist[width:width + 8, :] = jnp.zeros((8, LANES), F32)
    copies[0].wait()
    copies[1].wait()
    lane = lax.broadcasted_iota(jnp.int32, (1, LANES), 1)

    def source_step(g, carry):
        low, high = meta[g, 8, me], meta[g, 8, me + 1]
        scale = scale_ref[pl.ds(g, 1), :]

        def eight(q, c):
            factor = jnp.where(lane // rows == lax.shift_right_logical(q, 5), scale, 0.0)
            row = jnp.bitwise_and(q, 31) * 8
            at = [meta[g, lax.shift_right_logical(q, 4), jnp.bitwise_and(q, 15) * 8 + s] for s in range(8)]
            new = [hist[pl.ds(at[s], 1), :] + gath[g, pl.ds(row + s, 1), :] * factor for s in range(8)]
            for s in range(8):
                hist[pl.ds(at[s], 1), :] = new[s]
            return c

        lax.fori_loop(lax.shift_right_logical(low, 3), lax.shift_right_logical(high + 7, 3), eight, 0)
        return carry

    lax.fori_loop(0, group, source_step, 0)
    copies[2].wait()
    peak = stat_ref[0:rows]
    share = stat_ref[rows:2 * rows]

    def out_step(i, carry):
        for u in range(8):
            at = pl.ds(pl.multiple_of((i * 8 + u) * LANES, LANES), LANES)
            turned = hist[at, :].T
            knn = (turned[0:rows] + turned[rows:2 * rows]) + (turned[2 * rows:3 * rows] + turned[3 * rows:4 * rows])
            out_ref[:, at] = jnp.log(knn + jnp.exp(logits[:, at] - peak) * share)
        return carry

    lax.fori_loop(0, width // LANES // 8, out_step, 0)


def solution(mesh):
    group = mesh.shape['model']

    def local_step(hidden, w_local, keys_local, tok_local, bounds_local, temperature, mix_weight):
        rows, dim = hidden.shape
        width = w_local.shape[1]
        store = keys_local.shape[0]
        quarter = store // 4
        chips = group // 2
        vmem = pl.BlockSpec(memory_space=pltpu.VMEM)
        smem = pl.BlockSpec(memory_space=pltpu.SMEM)
        hbm = pl.BlockSpec(memory_space=pltpu.HBM)
        dma = pltpu.SemaphoreType.DMA
        gath_shape = (group, quarter + EXTRA, LANES)
        meta_shape = (group, 16, LANES)
        gath, logits, meta, scale, stat = pl.pallas_call(
            functools.partial(score_kernel, group),
            out_shape=(jax.ShapeDtypeStruct(gath_shape, F32), jax.ShapeDtypeStruct((rows, width), F32),
                       jax.ShapeDtypeStruct(meta_shape, jnp.int32), jax.ShapeDtypeStruct((group, LANES), F32),
                       jax.ShapeDtypeStruct((2 * rows, LANES), F32)),
            in_specs=[vmem, vmem, vmem, smem, smem, hbm, hbm],
            out_specs=(hbm, hbm, hbm, vmem, vmem),
            scratch_shapes=[
                pltpu.VMEM((4, quarter, dim), jnp.bfloat16),
                pltpu.VMEM((SLOTS, dim, BLOCK), jnp.bfloat16),
                pltpu.VMEM(gath_shape, F32),
                pltpu.VMEM((quarter, LANES), F32),
                pltpu.VMEM(meta_shape, jnp.int32),
                pltpu.VMEM((rows, width), F32),
                pltpu.VMEM((rows, LANES), F32),
                pltpu.VMEM((rows, LANES), F32),
                pltpu.VMEM((group, 1, LANES), F32),
                dma((4,)), dma((SLOTS,)), dma((6,)),
                dma((chips,)), dma((chips,)), dma((chips,)), dma((chips,)),
                dma((chips, 2)), dma((chips, 2)),
                dma((group,)), dma((group,)),
            ],
            compiler_params=pltpu.CompilerParams(collective_id=0, has_side_effects=True, vmem_limit_bytes=VMEM_BYTES),
            name='score_gather_head',
        )(hidden, tok_local.reshape(store // LANES, LANES), bounds_local, temperature.reshape(1),
          mix_weight.reshape(1), keys_local, w_local)
        return mix_call(group, rows, width, meta, gath, logits, scale, stat)

    return jax.shard_map(local_step, mesh=mesh,
                         in_specs=(P('data', None), P(None, 'model'), P('model', None), P('model'),
                                   P('model', None), P(), P()),
                         out_specs=P('data', 'model'), check_vma=False)


def mix_call(group, rows, width, meta, gath, logits, scale, stat):
    vmem = pl.BlockSpec(memory_space=pltpu.VMEM)
    hbm = pl.BlockSpec(memory_space=pltpu.HBM)
    return pl.pallas_call(
        functools.partial(mix_kernel, group),
        out_shape=jax.ShapeDtypeStruct((rows, width), F32),
        in_specs=[hbm, hbm, hbm, vmem, vmem],
        out_specs=vmem,
        scratch_shapes=[
            pltpu.SMEM(meta.shape, jnp.int32),
            pltpu.VMEM(gath.shape, F32),
            pltpu.VMEM((rows, width), F32),
            pltpu.VMEM((width + 8, LANES), F32),
            pltpu.SemaphoreType.DMA((3,)),
        ],
        compiler_params=pltpu.CompilerParams(vmem_limit_bytes=VMEM_BYTES),
        name='bin_mix',
    )(meta, gath, logits, scale, stat)
```

```python
import functools

import jax
import jax.numpy as jnp
from jax import lax
from jax.experimental import pallas as pl
from jax.experimental.pallas import tpu as pltpu
from jax.sharding import PartitionSpec as P

MESH_ID = pl.DeviceIdType.MESH
LANES = 128
BLOCK = 256
SLOTS = 16
F32 = jnp.float32
LOWEST = float(jnp.finfo(jnp.float32).min)
VMEM_BYTES = 64 * 1024 * 1024 - 65536
EXTRA = 16


def lane_groups(x, op):
    x = op(x, pltpu.roll(x, 64, 1))
    return op(x, pltpu.roll(x, 32, 1))


def score_kernel(group, hid_ref, tok_ref, rb_ref, tau_ref, lam_ref, keys_ref, w_ref,
                 gath_out, logit_out, meta_out, scale_out, stat_out,
                 kbuf, wbuf, gath, toks, meta, logits, mrun, srun, stats,
                 ksem, wsem, osem, rs, rr, ls, lr, ps, pr, ss, sr):
    me = lax.axis_index('model')
    chips = group // 2
    chip, core = me // 2, me % 2
    partner = me + 1 - 2 * core
    right = ((chip + 1) % chips) * 2 + core
    left = ((chip + chips - 1) % chips) * 2 + core
    rows, dim = hid_ref.shape
    quarter = kbuf.shape[1]
    half = (quarter + EXTRA) // 2
    width = logits.shape[1]
    blocks = width // BLOCK
    far = chips // 2
    extra = quarter + 8

    barrier = pltpu.get_barrier_semaphore()
    for p in range(1, group):
        pl.semaphore_signal(barrier, inc=1, device_id={'model': (me + p) % group}, device_id_type=MESH_ID)

    def key_copy(c):
        return pltpu.make_async_copy(keys_ref.at[pl.ds(pl.multiple_of(c * quarter, quarter), quarter)],
                                     kbuf.at[c], ksem.at[c])

    def w_copy(i):
        slot = lax.rem(i, SLOTS)
        return pltpu.make_async_copy(w_ref.at[:, pl.ds(pl.multiple_of(i * BLOCK, BLOCK), BLOCK)],
                                     wbuf.at[slot], wsem.at[slot])

    for c in range(4):
        key_copy(c).start()
    mrun[...] = jnp.full(mrun.shape, LOWEST, F32)
    srun[...] = jnp.zeros(srun.shape, F32)
    tok = tok_ref[...].astype(F32)
    gath[me, pl.ds(quarter, 8), :] = tok
    gath[me, pl.ds(extra, 8), :] = jnp.zeros((8, LANES), F32)
    gath[me, pl.ds(extra, 1), 0:rb_ref.shape[1]] = rb_ref[...].astype(F32)
    for h in range(2):
        toks[h * LANES:(h + 1) * LANES, :] = jnp.concatenate(
            [jnp.broadcast_to(tok[2 * k + h:2 * k + h + 1], (rows, LANES)) for k in range(4)], axis=0).T

    lane = lax.broadcasted_iota(jnp.int32, (quarter, LANES), 1)
    gath[me, 0:quarter, :] = jnp.zeros((quarter, LANES), F32)

    def score_step(c, carry):
        key_copy(c).wait()
        for u in range(SLOTS // 4):
            w_copy(c * (SLOTS // 4) + u).start()
        norm = jnp.zeros((quarter, LANES), F32)
        for t in range(dim // LANES):
            x = kbuf[c, :, t * LANES:(t + 1) * LANES].astype(F32)
            norm = norm + x * x
        norm = jnp.sum(norm, axis=1, keepdims=True)
        hid4 = jnp.concatenate([hid_ref[...]] * 4, axis=0)
        dot = lax.dot_general(kbuf[c], hid4, (((1,), (1,)), ((), ())), preferred_element_type=F32)
        score = (2.0 * dot - norm) / tau_ref[0]
        score = jnp.where(lane // rows == c, score, gath[me, 0:quarter, :])
        gath[me, 0:quarter, :] = score
        return carry

    lax.fori_loop(0, 4, score_step, 0)

    top = functools.reduce(jnp.maximum, [gath[me, r * 8:r * 8 + 8, :] for r in range(quarter // 8)])
    top = lane_groups(jnp.broadcast_to(jnp.max(top, axis=0, keepdims=True), (8, LANES)), jnp.maximum)
    sub = lax.broadcasted_iota(jnp.int32, (8, LANES), 0)

    def exp_step(r, total):
        at = pl.ds(pl.multiple_of(r * 8, 8), 8)
        e = jnp.exp(gath[me, at, :] - top)
        total = total + e
        ids = toks[at, :]
        last = (ids != pltpu.roll(ids, 7, 0)) | (sub == 7)
        for d in (1, 2, 4):
            same = (ids == pltpu.roll(ids, d, 0)) & (sub >= d)
            e = e + jnp.where(same, pltpu.roll(e, d, 0), 0.0)
        gath[me, at, :] = jnp.where(last, e, 0.0)
        return total

    total = lax.fori_loop(0, quarter // 8, exp_step, jnp.zeros((8, LANES), F32), unroll=8)
    total = lane_groups(jnp.broadcast_to(jnp.sum(total, axis=0, keepdims=True), (8, LANES)), jnp.add)
    gath[me, pl.ds(extra + 1, 1), :] = top[0:1]
    gath[me, pl.ds(extra + 2, 1), :] = total[0:1]

    pl.semaphore_wait(barrier, group - 1)

    def remote(ref, slot, part, send, recv, target):
        view = ref.at[slot] if part is None else ref.at[slot, pl.ds(part * half, half)]
        return pltpu.make_async_remote_copy(view, view, send, recv, device_id={'model': target},
                                            device_id_type=MESH_ID)

    def origin(step, sign):
        return ((chip + chips + sign * step) % chips) * 2 + core

    def right_piece(s, h):
        return remote(gath, origin(s - 1, -1), h, rs.at[2 * s - 2 + h], rr.at[2 * s - 2 + h], right)

    def right_landed(s, h):
        return remote(gath, origin(s, -1), h, rs.at[2 * s - 2 + h], rr.at[2 * s - 2 + h], right)

    def left_piece(s, h):
        return remote(gath, origin(s - 1, 1), h, ls.at[2 * s - 2 + h], lr.at[2 * s - 2 + h], left)

    def left_landed(s, h):
        return remote(gath, origin(s, 1), h, ls.at[2 * s - 2 + h], lr.at[2 * s - 2 + h], left)

    def across(step, h, q):
        return remote(gath, origin(step, -1), h, ps.at[q, h], pr.at[q, h], partner)

    def across_landed(step, h, q):
        slot = origin(step, -1) + 1 - 2 * core
        return remote(gath, slot, h, ps.at[q, h], pr.at[q, h], partner)

    for h in range(2):
        right_piece(1, h).start()
        left_piece(1, h).start()
    for h in range(2):
        across(0, h, 0).start()

    right_order = [(s, h) for s in range(1, far) for h in range(2)] + [(far, 0)]
    left_order = [(s, h) for s in range(1, far) for h in range(2)] + [(far, 1)]

    def ring_event(e):
        s, h = right_order[e]
        right_landed(s, h).wait_recv()
        if (s + 1, h) in right_order:
            right_piece(s + 1, h).start()
        across(s, h, s).start()
        s, h = left_order[e]
        left_landed(s, h).wait_recv()
        if (s + 1, h) in left_order:
            left_piece(s + 1, h).start()
        across(chips - s, h, chips - s).start()

    gath_copy = pltpu.make_async_copy(gath, gath_out, osem.at[0])
    meta_copy = pltpu.make_async_copy(meta, meta_out, osem.at[1])

    def gathered():
        for q in range(chips):
            for h in range(2):
                across_landed(q, h, q).wait_recv()
        gath_copy.start()
        tile_lane = lax.broadcasted_iota(jnp.int32, (8, LANES), 1)
        place = lax.broadcasted_iota(jnp.int32, (8, LANES), 0) * LANES + tile_lane
        high = functools.reduce(jnp.maximum, [gath[g, extra + 1:extra + 2, :] for g in range(group)])
        shares = [jnp.exp(gath[g, extra + 1:extra + 2, :] - high) for g in range(group)]
        whole = sum(gath[g, extra + 2:extra + 3, :] * shares[g] for g in range(group))
        for g in range(group):
            scale_out[g:g + 1, :] = shares[g] * (lam_ref[0] / whole)

        def index_step(g, carry):
            bounds = gath[g, extra:extra + 8, :]
            first = jnp.sum(jnp.where(tile_lane == me, bounds, 0.0), axis=1, keepdims=True)[0:1].astype(jnp.int32)
            after = jnp.sum(jnp.where(tile_lane == me + 1, bounds, 0.0), axis=1, keepdims=True)[0:1].astype(jnp.int32)
            ids = gath[g, quarter:quarter + 8, :].astype(jnp.int32)
            meta[g, 0:8, :] = jnp.where((place >= first) & (place < after), ids - me * width, width)
            meta[g, 8:16, :] = bounds.astype(jnp.int32)
            return carry

        lax.fori_loop(0, group, index_step, 0, unroll=4)
        meta_copy.start()

    def block_stats(i, keep):
        parts = [logits[:, pl.ds(pl.multiple_of(i * BLOCK, BLOCK) + t * LANES, LANES)] for t in range(BLOCK // LANES)]
        old = mrun[...]
        new = functools.reduce(jnp.maximum, parts, old)
        srun[...] = sum((jnp.exp(x - new) for x in parts), srun[...] * jnp.exp(old - new)) * keep
        mrun[...] = new

    bands = 4
    band = width // bands

    def logit_copy(b):
        at = pl.ds(b * band, band)
        return pltpu.make_async_copy(logits.at[:, at], logit_out.at[:, at], osem.at[2 + b])

    logits[:, 0:BLOCK] = jnp.full((rows, BLOCK), LOWEST, F32)

    def w_step(i, carry):
        slot = lax.rem(i, SLOTS)
        w_copy(i).wait()
        block_stats(jnp.maximum(i - 1, 0), jnp.where(i > 0, 1.0, 0.0))
        acc = jnp.dot(hid_ref[...], wbuf[slot], preferred_element_type=F32)
        logits[:, pl.ds(pl.multiple_of(i * BLOCK, BLOCK), BLOCK)] = acc

        @pl.when(i + SLOTS < blocks)
        def _():
            w_copy(i + SLOTS).start()

        for e in range(len(right_order)):
            pl.when(i == 3 + 3 * e)(functools.partial(ring_event, e))
        pl.when(i == 4 + 3 * len(right_order))(gathered)
        for b in range(bands - 1):
            pl.when(i == (b + 1) * (blocks // bands))(logit_copy(b).start)
        return carry

    lax.fori_loop(0, blocks, w_step, 0)
    block_stats(blocks - 1, 1.0)
    logit_copy(bands - 1).start()

    peak = jnp.max(mrun[...], axis=1, keepdims=True)
    tot = jnp.sum(srun[...] * jnp.exp(mrun[...] - peak), axis=1, keepdims=True)
    pad = jnp.zeros((64 - rows, LANES), F32)
    square = jnp.concatenate([jnp.broadcast_to(peak, (rows, LANES)), pad, jnp.broadcast_to(tot, (rows, LANES)), pad],
                             axis=0)
    stats[me] = square.T[0:1]

    def stat_copy(p, slot):
        return remote(stats, slot, None, ss.at[p], sr.at[p], (me + p) % group)

    for p in range(1, group):
        stat_copy(p, me).start()
    for p in range(1, group):
        stat_copy(p, (me + group - p) % group).wait_recv()

    row_lane = lax.broadcasted_iota(jnp.int32, (1, LANES), 1)
    every = [stats[g] for g in range(group)]
    high = functools.reduce(jnp.maximum, every)
    total = jnp.zeros((1, LANES), F32)
    for one in every:
        moved = pltpu.roll(jnp.broadcast_to(one, (8, LANES)), 64, 1)[0:1]
        total = total + moved * jnp.exp(jnp.where(row_lane < rows, one - high, 0.0))
    share = (1.0 - lam_ref[0]) / jnp.where(row_lane < rows, total, 1.0)
    stat_out[0:rows] = jnp.broadcast_to(high, (LANES, LANES)).T[0:rows]
    stat_out[rows:2 * rows] = jnp.broadcast_to(share, (LANES, LANES)).T[0:rows]

    for s, h in right_order:
        right_piece(s, h).wait_send()
    for s, h in left_order:
        left_piece(s, h).wait_send()
    for q in range(chips):
        for h in range(2):
            across(q, h, q).wait_send()
    for p in range(1, group):
        stat_copy(p, me).wait_send()
    gath_copy.wait()
    meta_copy.wait()
    for b in range(bands):
        logit_copy(b).wait()


def mix_kernel(group, meta_hbm, gath_hbm, logit_hbm, scale_ref, stat_ref, out_hbm,
               meta, gath, logits, hist, sems, gsem, osem):
    me = lax.axis_index('model')
    rows, width = logits.shape
    span = meta.shape[0] // group
    bounds = span // 2
    bands = osem.shape[0]
    band = width // bands
    meta_copy = pltpu.make_async_copy(meta_hbm, meta, sems.at[0])
    logit_copy = pltpu.make_async_copy(logit_hbm, logits, sems.at[1])

    def gath_copy(g):
        return pltpu.make_async_copy(gath_hbm.at[g], gath.at[g], gsem.at[g])

    meta_copy.start()
    for g in range(group):
        gath_copy(g).start()
    logit_copy.start()

    def zero_step(i, carry):
        hist[pl.ds(pl.multiple_of(i * LANES, LANES), LANES), :] = jnp.zeros((LANES, LANES), F32)
        return carry

    lax.fori_loop(0, width // LANES, zero_step, 0)
    hist[width:width + 8, :] = jnp.zeros((8, LANES), F32)
    meta_copy.wait()
    lane = lax.broadcasted_iota(jnp.int32, (1, LANES), 1)

    def source_step(g, carry):
        start = g * span
        low, high = meta[start + bounds + me], meta[start + bounds + me + 1]
        scale = scale_ref[pl.ds(g, 1), :]
        gath_copy(g).wait()

        def eight(q, c):
            factor = jnp.where(lane // rows == lax.shift_right_logical(q, 5), scale, 0.0)
            row = jnp.bitwise_and(q, 31) * 8
            first = start + q * 8
            at = [meta[first + s] for s in range(8)]
            new = [hist[pl.ds(at[s], 1), :] + gath[g, pl.ds(row + s, 1), :] * factor for s in range(8)]
            for s in range(8):
                hist[pl.ds(at[s], 1), :] = new[s]
            return c

        lax.fori_loop(lax.shift_right_logical(low, 3), lax.shift_right_logical(high + 7, 3), eight, 0)
        return carry

    lax.fori_loop(0, group, source_step, 0)
    logit_copy.wait()
    peak = stat_ref[0:rows]
    share = stat_ref[rows:2 * rows]
    steps = 8

    def out_copy(b):
        at = pl.ds(pl.multiple_of(b * band, band), band)
        return pltpu.make_async_copy(logits.at[:, at], out_hbm.at[:, at], osem.at[b])

    def out_step(i, carry):
        for u in range(steps):
            at = pl.ds(pl.multiple_of(i * band + u * LANES, LANES), LANES)
            turned = hist[at, :].T
            knn = (turned[0:rows] + turned[rows:2 * rows]) + (turned[2 * rows:3 * rows] + turned[3 * rows:4 * rows])
            logits[:, at] = jnp.log(knn + jnp.exp(logits[:, at] - peak) * share)
        out_copy(i).start()
        return carry

    lax.fori_loop(0, bands, out_step, 0)
    for b in range(bands):
        out_copy(b).wait()


def solution(mesh):
    group = mesh.shape['model']

    def local_step(hidden, w_local, keys_local, tok_local, bounds_local, temperature, mix_weight):
        rows, dim = hidden.shape
        width = w_local.shape[1]
        store = keys_local.shape[0]
        quarter = store // 4
        chips = group // 2
        vmem = pl.BlockSpec(memory_space=pltpu.VMEM)
        smem = pl.BlockSpec(memory_space=pltpu.SMEM)
        hbm = pl.BlockSpec(memory_space=pltpu.HBM)
        dma = pltpu.SemaphoreType.DMA
        gath_shape = (group, quarter + EXTRA, LANES)
        meta_shape = (group, 16, LANES)
        gath, logits, meta, scale, stat = pl.pallas_call(
            functools.partial(score_kernel, group),
            out_shape=(jax.ShapeDtypeStruct(gath_shape, F32), jax.ShapeDtypeStruct((rows, width), F32),
                       jax.ShapeDtypeStruct(meta_shape, jnp.int32), jax.ShapeDtypeStruct((group, LANES), F32),
                       jax.ShapeDtypeStruct((2 * rows, LANES), F32)),
            in_specs=[vmem, vmem, vmem, smem, smem, hbm, hbm],
            out_specs=(hbm, hbm, hbm, vmem, vmem),
            scratch_shapes=[
                pltpu.VMEM((4, quarter, dim), jnp.bfloat16),
                pltpu.VMEM((SLOTS, dim, BLOCK), jnp.bfloat16),
                pltpu.VMEM(gath_shape, F32),
                pltpu.VMEM((quarter, LANES), F32),
                pltpu.VMEM(meta_shape, jnp.int32),
                pltpu.VMEM((rows, width), F32),
                pltpu.VMEM((rows, LANES), F32),
                pltpu.VMEM((rows, LANES), F32),
                pltpu.VMEM((group, 1, LANES), F32),
                dma((4,)), dma((SLOTS,)), dma((6,)),
                dma((chips,)), dma((chips,)), dma((chips,)), dma((chips,)),
                dma((chips, 2)), dma((chips, 2)),
                dma((group,)), dma((group,)),
            ],
            compiler_params=pltpu.CompilerParams(collective_id=0, has_side_effects=True, vmem_limit_bytes=VMEM_BYTES),
            name='score_gather_head',
        )(hidden, tok_local.reshape(store // LANES, LANES), bounds_local, temperature.reshape(1),
          mix_weight.reshape(1), keys_local, w_local)
        return mix_call(group, rows, width, meta, gath, logits, scale, stat)

    return jax.shard_map(local_step, mesh=mesh,
                         in_specs=(P('data', None), P(None, 'model'), P('model', None), P('model'),
                                   P('model', None), P(), P()),
                         out_specs=P('data', 'model'), check_vma=False)


def mix_call(group, rows, width, meta, gath, logits, scale, stat):
    vmem = pl.BlockSpec(memory_space=pltpu.VMEM)
    hbm = pl.BlockSpec(memory_space=pltpu.HBM)
    dma = pltpu.SemaphoreType.DMA
    return pl.pallas_call(
        functools.partial(mix_kernel, group),
        out_shape=jax.ShapeDtypeStruct((rows, width), F32),
        in_specs=[hbm, hbm, hbm, vmem, vmem],
        out_specs=hbm,
        scratch_shapes=[
            pltpu.SMEM((meta.size,), jnp.int32),
            pltpu.VMEM(gath.shape, F32),
            pltpu.VMEM((rows, width), F32),
            pltpu.VMEM((width + 8, LANES), F32),
            dma((2,)), dma((group,)), dma((width // (8 * LANES),)),
        ],
        compiler_params=pltpu.CompilerParams(vmem_limit_bytes=VMEM_BYTES),
        name='bin_mix',
    )(meta.reshape(meta.size), gath, logits, scale, stat)
```

```python
import functools

import jax
import jax.numpy as jnp
from jax import lax
from jax.experimental import pallas as pl
from jax.experimental.pallas import tpu as pltpu
from jax.sharding import PartitionSpec as P

MESH_ID = pl.DeviceIdType.MESH
LANES = 128
BLOCK = 256
SLOTS = 14
GROUP = 16
F32 = jnp.float32
LOWEST = float(jnp.finfo(jnp.float32).min)
VMEM_BYTES = 64 * 1024 * 1024 - 65536
EXTRA = 16


def lane_groups(x, op):
    x = op(x, pltpu.roll(x, 64, 1))
    return op(x, pltpu.roll(x, 32, 1))


def score_kernel(group, hid_ref, tok_ref, rb_ref, tau_ref, lam_ref, keys_ref, w_ref,
                 gath_out, logit_out, meta_out, scale_out, stat_out,
                 kbuf, wbuf, gath, logits, toks, meta, mrun, srun, stats,
                 ksem, wsem, osem, rs, rr, ls, lr, ps, pr, ss, sr):
    me = lax.axis_index('model')
    chips = group // 2
    chip, core = me // 2, me % 2
    partner = me + 1 - 2 * core
    right = ((chip + 1) % chips) * 2 + core
    left = ((chip + chips - 1) % chips) * 2 + core
    rows, dim = hid_ref.shape
    quarter = kbuf.shape[1]
    half = (quarter + EXTRA) // 2
    width = logits.shape[1]
    blocks = width // BLOCK
    far = chips // 2
    extra = quarter + 8

    barrier = pltpu.get_barrier_semaphore()
    for p in range(1, group):
        pl.semaphore_signal(barrier, inc=1, device_id={'model': (me + p) % group}, device_id_type=MESH_ID)

    def key_copy(c):
        return pltpu.make_async_copy(keys_ref.at[pl.ds(pl.multiple_of(c * quarter, quarter), quarter)],
                                     kbuf.at[c], ksem.at[c])

    def w_copy(i):
        slot = lax.rem(i, SLOTS)
        return pltpu.make_async_copy(w_ref.at[:, pl.ds(pl.multiple_of(i * BLOCK, BLOCK), BLOCK)],
                                     wbuf.at[slot], wsem.at[slot])

    for c in range(4):
        key_copy(c).start()
    mrun[...] = jnp.full(mrun.shape, LOWEST, F32)
    srun[...] = jnp.zeros(srun.shape, F32)
    tok = tok_ref[...].astype(F32)
    gath[me, pl.ds(quarter, 8), :] = tok
    gath[me, pl.ds(extra, 8), :] = jnp.zeros((8, LANES), F32)
    gath[me, pl.ds(extra, 1), 0:rb_ref.shape[1]] = rb_ref[...].astype(F32)
    for h in range(2):
        toks[h * LANES:(h + 1) * LANES, :] = jnp.concatenate(
            [jnp.broadcast_to(tok[2 * k + h:2 * k + h + 1], (rows, LANES)) for k in range(4)], axis=0).T

    lane = lax.broadcasted_iota(jnp.int32, (quarter, LANES), 1)
    gath[me, 0:quarter, :] = jnp.zeros((quarter, LANES), F32)

    def score_step(c, carry):
        key_copy(c).wait()
        for u in range(3):
            w_copy(3 * c + u).start()
        norm = jnp.zeros((quarter, LANES), F32)
        for t in range(dim // LANES):
            x = kbuf[c, :, t * LANES:(t + 1) * LANES].astype(F32)
            norm = norm + x * x
        norm = jnp.sum(norm, axis=1, keepdims=True)
        hid4 = jnp.concatenate([hid_ref[...]] * 4, axis=0)
        dot = lax.dot_general(kbuf[c], hid4, (((1,), (1,)), ((), ())), preferred_element_type=F32)
        score = (2.0 * dot - norm) / tau_ref[0]
        score = jnp.where(lane // rows == c, score, gath[me, 0:quarter, :])
        gath[me, 0:quarter, :] = score
        return carry

    lax.fori_loop(0, 4, score_step, 0)
    for i in range(12, SLOTS):
        w_copy(i).start()

    top = functools.reduce(jnp.maximum, [gath[me, r * 8:r * 8 + 8, :] for r in range(quarter // 8)])
    top = lane_groups(jnp.broadcast_to(jnp.max(top, axis=0, keepdims=True), (8, LANES)), jnp.maximum)
    sub = lax.broadcasted_iota(jnp.int32, (8, LANES), 0)

    def run_sums(e, ids):
        for d in (1, 2, 4):
            e = e + jnp.where((ids == pltpu.roll(ids, d, 0)) & (sub >= d), pltpu.roll(e, d, 0), 0.0)
        return e

    def exp_step(r, total):
        at = [pl.ds(pl.multiple_of(r * GROUP + 8 * u, 8), 8) for u in range(2)]
        e = [jnp.exp(gath[me, a, :] - top) for a in at]
        ids = [toks[a, :] for a in at]
        sums = [run_sums(e[u], ids[u]) for u in range(2)]
        spread = lambda x: jnp.broadcast_to(x, (8, LANES))
        sums[1] = sums[1] + jnp.where(ids[1] == spread(ids[0][7:8]), spread(sums[0][7:8]), 0.0)
        after = jnp.where(sub == 7, spread(ids[1][0:1]), pltpu.roll(ids[0], 7, 0))
        gath[me, at[0], :] = jnp.where(ids[0] != after, sums[0], 0.0)
        gath[me, at[1], :] = jnp.where((ids[1] != pltpu.roll(ids[1], 7, 0)) | (sub == 7), sums[1], 0.0)
        return total + (e[0] + e[1])

    total = lax.fori_loop(0, quarter // GROUP, exp_step, jnp.zeros((8, LANES), F32), unroll=4)
    total = lane_groups(jnp.broadcast_to(jnp.sum(total, axis=0, keepdims=True), (8, LANES)), jnp.add)
    gath[me, pl.ds(extra + 1, 1), :] = top[0:1]
    gath[me, pl.ds(extra + 2, 1), :] = total[0:1]

    pl.semaphore_wait(barrier, group - 1)

    def remote(ref, slot, part, send, recv, target):
        view = ref.at[slot] if part is None else ref.at[slot, pl.ds(part * half, half)]
        return pltpu.make_async_remote_copy(view, view, send, recv, device_id={'model': target},
                                            device_id_type=MESH_ID)

    def origin(step, sign):
        return ((chip + chips + sign * step) % chips) * 2 + core

    def right_piece(s, h):
        return remote(gath, origin(s - 1, -1), h, rs.at[2 * s - 2 + h], rr.at[2 * s - 2 + h], right)

    def right_landed(s, h):
        return remote(gath, origin(s, -1), h, rs.at[2 * s - 2 + h], rr.at[2 * s - 2 + h], right)

    def left_piece(s, h):
        return remote(gath, origin(s - 1, 1), h, ls.at[2 * s - 2 + h], lr.at[2 * s - 2 + h], left)

    def left_landed(s, h):
        return remote(gath, origin(s, 1), h, ls.at[2 * s - 2 + h], lr.at[2 * s - 2 + h], left)

    def across(step, h, q):
        return remote(gath, origin(step, -1), h, ps.at[q, h], pr.at[q, h], partner)

    def across_landed(step, h, q):
        slot = origin(step, -1) + 1 - 2 * core
        return remote(gath, slot, h, ps.at[q, h], pr.at[q, h], partner)

    for h in range(2):
        right_piece(1, h).start()
        left_piece(1, h).start()
    for h in range(2):
        across(0, h, 0).start()

    right_order = [(s, h) for s in range(1, far) for h in range(2)] + [(far, 0)]
    left_order = [(s, h) for s in range(1, far) for h in range(2)] + [(far, 1)]

    def ring_event(e):
        s, h = right_order[e]
        right_landed(s, h).wait_recv()
        if (s + 1, h) in right_order:
            right_piece(s + 1, h).start()
        across(s, h, s).start()
        s, h = left_order[e]
        left_landed(s, h).wait_recv()
        if (s + 1, h) in left_order:
            left_piece(s + 1, h).start()
        across(chips - s, h, chips - s).start()

    meta_copy = pltpu.make_async_copy(meta, meta_out, osem.at[0])
    gath_copy = pltpu.make_async_copy(gath, gath_out, osem.at[1])

    def gathered():
        for q in range(chips):
            for h in range(2):
                across_landed(q, h, q).wait_recv()
        gath_copy.start()
        tile_lane = lax.broadcasted_iota(jnp.int32, (8, LANES), 1)
        place = lax.broadcasted_iota(jnp.int32, (8, LANES), 0) * LANES + tile_lane
        high = functools.reduce(jnp.maximum, [gath[g, extra + 1:extra + 2, :] for g in range(group)])
        shares = [jnp.exp(gath[g, extra + 1:extra + 2, :] - high) for g in range(group)]
        whole = sum(gath[g, extra + 2:extra + 3, :] * shares[g] for g in range(group))
        for g in range(group):
            scale_out[g:g + 1, :] = shares[g] * (lam_ref[0] / whole)

        def index_step(g, carry):
            bounds = gath[g, extra:extra + 8, :]
            first = jnp.sum(jnp.where(tile_lane == me, bounds, 0.0), axis=1, keepdims=True)[0:1].astype(jnp.int32)
            after = jnp.sum(jnp.where(tile_lane == me + 1, bounds, 0.0), axis=1, keepdims=True)[0:1].astype(jnp.int32)
            ids = gath[g, quarter:quarter + 8, :].astype(jnp.int32)
            meta[pl.ds(pl.multiple_of(8 * g, 8), 8), :] = jnp.where((place >= first) & (place < after),
                                                                    ids - me * width, width)
            return carry

        lax.fori_loop(0, group, index_step, 0, unroll=4)
        for g in range(group):
            meta[8 * group + g:8 * group + g + 1, :] = gath[g, extra:extra + 1, :].astype(jnp.int32)
        meta_copy.start()

    def block_stats(i, keep):
        parts = [logits[:, pl.ds(pl.multiple_of(i * BLOCK, BLOCK) + t * LANES, LANES)] for t in range(BLOCK // LANES)]
        old = mrun[...]
        new = functools.reduce(jnp.maximum, parts, old)
        srun[...] = sum((jnp.exp(x - new) for x in parts), srun[...] * jnp.exp(old - new)) * keep
        mrun[...] = new

    bands = 4
    band = width // bands

    def logit_copy(b):
        at = pl.ds(b * band, band)
        return pltpu.make_async_copy(logits.at[:, at], logit_out.at[:, at], osem.at[2 + b])

    logits[:, 0:BLOCK] = jnp.full((rows, BLOCK), LOWEST, F32)

    def w_step(i, carry):
        slot = lax.rem(i, SLOTS)
        w_copy(i).wait()
        block_stats(jnp.maximum(i - 1, 0), jnp.where(i > 0, 1.0, 0.0))
        acc = jnp.dot(hid_ref[...], wbuf[slot], preferred_element_type=F32)
        logits[:, pl.ds(pl.multiple_of(i * BLOCK, BLOCK), BLOCK)] = acc

        @pl.when(i + SLOTS < blocks)
        def _():
            w_copy(i + SLOTS).start()

        for e in range(len(right_order)):
            pl.when(i == 3 + 3 * e)(functools.partial(ring_event, e))
        pl.when(i == 4 + 3 * len(right_order))(gathered)
        for b in range(bands - 1):
            pl.when(i == (b + 1) * (blocks // bands))(logit_copy(b).start)
        return carry

    lax.fori_loop(0, blocks, w_step, 0)
    block_stats(blocks - 1, 1.0)
    logit_copy(bands - 1).start()

    peak = jnp.max(mrun[...], axis=1, keepdims=True)
    tot = jnp.sum(srun[...] * jnp.exp(mrun[...] - peak), axis=1, keepdims=True)
    pad = jnp.zeros((64 - rows, LANES), F32)
    square = jnp.concatenate([jnp.broadcast_to(peak, (rows, LANES)), pad, jnp.broadcast_to(tot, (rows, LANES)), pad],
                             axis=0)
    stats[me] = square.T[0:1]

    def stat_copy(p, slot):
        return remote(stats, slot, None, ss.at[p], sr.at[p], (me + p) % group)

    for p in range(1, group):
        stat_copy(p, me).start()
    for p in range(1, group):
        stat_copy(p, (me + group - p) % group).wait_recv()

    row_lane = lax.broadcasted_iota(jnp.int32, (1, LANES), 1)
    every = [stats[g] for g in range(group)]
    high = functools.reduce(jnp.maximum, every)
    total = jnp.zeros((1, LANES), F32)
    for one in every:
        moved = pltpu.roll(jnp.broadcast_to(one, (8, LANES)), 64, 1)[0:1]
        total = total + moved * jnp.exp(jnp.where(row_lane < rows, one - high, 0.0))
    share = (1.0 - lam_ref[0]) / jnp.where(row_lane < rows, total, 1.0)
    stat_out[0:rows] = jnp.broadcast_to(high, (LANES, LANES)).T[0:rows]
    stat_out[rows:2 * rows] = jnp.broadcast_to(share, (LANES, LANES)).T[0:rows]

    for s, h in right_order:
        right_piece(s, h).wait_send()
    for s, h in left_order:
        left_piece(s, h).wait_send()
    for q in range(chips):
        for h in range(2):
            across(q, h, q).wait_send()
    for p in range(1, group):
        stat_copy(p, me).wait_send()
    meta_copy.wait()
    gath_copy.wait()
    for b in range(bands):
        logit_copy(b).wait()


def mix_kernel(group, meta_hbm, gath_hbm, logit_hbm, scale_ref, stat_ref, out_hbm,
               meta, gath, logits, hist, sems, gsem, osem):
    me = lax.axis_index('model')
    rows, width = logits.shape
    span = meta.shape[0] // (group * 9) * 8
    bands = osem.shape[0]
    band = width // bands
    meta_copy = pltpu.make_async_copy(meta_hbm, meta, sems.at[0])
    logit_copy = pltpu.make_async_copy(logit_hbm, logits, sems.at[1])

    def gath_copy(g):
        return pltpu.make_async_copy(gath_hbm.at[g], gath.at[g], gsem.at[g])

    meta_copy.start()
    for g in range(group):
        gath_copy(g).start()
    logit_copy.start()

    def zero_step(i, carry):
        hist[pl.ds(pl.multiple_of(i * LANES, LANES), LANES), :] = jnp.zeros((LANES, LANES), F32)
        return carry

    lax.fori_loop(0, width // LANES, zero_step, 0)
    hist[width:width + 8, :] = jnp.zeros((8, LANES), F32)
    meta_copy.wait()
    lane = lax.broadcasted_iota(jnp.int32, (1, LANES), 1)

    def source_step(g, carry):
        start = g * span
        edge = group * span + g * LANES + me
        low, high = meta[edge], meta[edge + 1]
        scale = scale_ref[pl.ds(g, 1), :]

        gath_copy(g).wait()
        begin, end = lax.shift_right_logical(low, 4), lax.shift_right_logical(high + GROUP - 1, 4)

        def table_rows(q):
            return tuple(meta[start + q * GROUP + s] for s in range(GROUP))

        def bin_step(q, at):
            factor = jnp.where(lane // rows == lax.shift_right_logical(q, 4), scale, 0.0)
            row = jnp.bitwise_and(q, 15) * GROUP
            new = [hist[pl.ds(at[s], 1), :] + gath[g, pl.ds(row + s, 1), :] * factor for s in range(GROUP)]
            for s in range(GROUP):
                hist[pl.ds(at[s], 1), :] = new[s]
            return table_rows(q + 1)

        lax.fori_loop(begin, end, bin_step, table_rows(begin))
        return carry

    lax.fori_loop(0, group, source_step, 0)
    logit_copy.wait()
    peak = stat_ref[0:rows]
    share = stat_ref[rows:2 * rows]
    steps = 8

    def out_copy(b):
        at = pl.ds(pl.multiple_of(b * band, band), band)
        return pltpu.make_async_copy(logits.at[:, at], out_hbm.at[:, at], osem.at[b])

    def out_step(i, carry):
        for u in range(steps):
            at = pl.ds(pl.multiple_of(i * band + u * LANES, LANES), LANES)
            turned = hist[at, :].T
            knn = (turned[0:rows] + turned[rows:2 * rows]) + (turned[2 * rows:3 * rows] + turned[3 * rows:4 * rows])
            logits[:, at] = jnp.log(knn + jnp.exp(logits[:, at] - peak) * share)
        out_copy(i).start()
        return carry

    lax.fori_loop(0, bands, out_step, 0)
    for b in range(bands):
        out_copy(b).wait()


def solution(mesh):
    group = mesh.shape['model']

    def local_step(hidden, w_local, keys_local, tok_local, bounds_local, temperature, mix_weight):
        rows, dim = hidden.shape
        width = w_local.shape[1]
        store = keys_local.shape[0]
        quarter = store // 4
        chips = group // 2
        vmem = pl.BlockSpec(memory_space=pltpu.VMEM)
        smem = pl.BlockSpec(memory_space=pltpu.SMEM)
        hbm = pl.BlockSpec(memory_space=pltpu.HBM)
        dma = pltpu.SemaphoreType.DMA
        gath_shape = (group, quarter + EXTRA, LANES)
        meta_shape = (group * 9, LANES)
        gath, logits, meta, scale, stat = pl.pallas_call(
            functools.partial(score_kernel, group),
            out_shape=(jax.ShapeDtypeStruct(gath_shape, F32), jax.ShapeDtypeStruct((rows, width), F32),
                       jax.ShapeDtypeStruct(meta_shape, jnp.int32), jax.ShapeDtypeStruct((group, LANES), F32),
                       jax.ShapeDtypeStruct((2 * rows, LANES), F32)),
            in_specs=[vmem, vmem, vmem, smem, smem, hbm, hbm],
            out_specs=(hbm, hbm, hbm, vmem, vmem),
            scratch_shapes=[
                pltpu.VMEM((4, quarter, dim), jnp.bfloat16),
                pltpu.VMEM((SLOTS, dim, BLOCK), jnp.bfloat16),
                pltpu.VMEM(gath_shape, F32),
                pltpu.VMEM((rows, width), F32),
                pltpu.VMEM((quarter, LANES), F32),
                pltpu.VMEM(meta_shape, jnp.int32),
                pltpu.VMEM((rows, LANES), F32),
                pltpu.VMEM((rows, LANES), F32),
                pltpu.VMEM((group, 1, LANES), F32),
                dma((4,)), dma((SLOTS,)), dma((6,)),
                dma((chips,)), dma((chips,)), dma((chips,)), dma((chips,)),
                dma((chips, 2)), dma((chips, 2)),
                dma((group,)), dma((group,)),
            ],
            compiler_params=pltpu.CompilerParams(collective_id=0, has_side_effects=True, vmem_limit_bytes=VMEM_BYTES),
            name='score_gather_head',
        )(hidden, tok_local.reshape(store // LANES, LANES), bounds_local, temperature.reshape(1),
          mix_weight.reshape(1), keys_local, w_local)
        return mix_call(group, rows, width, meta, gath, logits, scale, stat)

    return jax.shard_map(local_step, mesh=mesh,
                         in_specs=(P('data', None), P(None, 'model'), P('model', None), P('model'),
                                   P('model', None), P(), P()),
                         out_specs=P('data', 'model'), check_vma=False)


def mix_call(group, rows, width, meta, gath, logits, scale, stat):
    vmem = pl.BlockSpec(memory_space=pltpu.VMEM)
    hbm = pl.BlockSpec(memory_space=pltpu.HBM)
    dma = pltpu.SemaphoreType.DMA
    return pl.pallas_call(
        functools.partial(mix_kernel, group),
        out_shape=jax.ShapeDtypeStruct((rows, width), F32),
        in_specs=[hbm, hbm, hbm, vmem, vmem],
        out_specs=hbm,
        scratch_shapes=[
            pltpu.SMEM((meta.size,), jnp.int32),
            pltpu.VMEM(gath.shape, F32),
            pltpu.VMEM((rows, width), F32),
            pltpu.VMEM((width + 8, LANES), F32),
            dma((2,)), dma((group,)), dma((width // (8 * LANES),)),
        ],
        compiler_params=pltpu.CompilerParams(vmem_limit_bytes=VMEM_BYTES),
        name='bin_mix',
    )(meta.reshape(meta.size), gath, logits, scale, stat)
```

```python
import functools

import jax
import jax.numpy as jnp
from jax import lax
from jax.experimental import pallas as pl
from jax.experimental.pallas import tpu as pltpu
from jax.sharding import PartitionSpec as P

MESH_ID = pl.DeviceIdType.MESH
LANES = 128
BLOCK = 256
SLOTS = 14
GROUP = 16
F32 = jnp.float32
LOWEST = float(jnp.finfo(jnp.float32).min)
VMEM_BYTES = 64 * 1024 * 1024 - 65536
EXTRA = 16


def lane_groups(x, op):
    x = op(x, pltpu.roll(x, 64, 1))
    return op(x, pltpu.roll(x, 32, 1))


def score_kernel(group, tau_ref, lam_ref, hid_hbm, tok_hbm, rb_hbm, keys_ref, w_ref,
                 gath_out, logit_out, meta_out, scale_hbm, stat_hbm,
                 hid_ref, tok_ref, rb_ref, scale_out, stat_out, kbuf, wbuf, gath, logits, toks, meta, mrun, srun, stats,
                 isem, ksem, wsem, osem, rs, rr, ls, lr, ps, pr, ss, sr):
    me = lax.axis_index('model')
    chips = group // 2
    chip, core = me // 2, me % 2
    partner = me + 1 - 2 * core
    right = ((chip + 1) % chips) * 2 + core
    left = ((chip + chips - 1) % chips) * 2 + core
    rows, dim = hid_ref.shape
    quarter = kbuf.shape[1]
    half = (quarter + EXTRA) // 2
    width = logits.shape[1]
    blocks = width // BLOCK
    far = chips // 2
    extra = quarter + 8

    def key_copy(c):
        return pltpu.make_async_copy(keys_ref.at[pl.ds(pl.multiple_of(c * quarter, quarter), quarter)],
                                     kbuf.at[c], ksem.at[c])

    def w_copy(i):
        slot = lax.rem(i, SLOTS)
        return pltpu.make_async_copy(w_ref.at[:, pl.ds(pl.multiple_of(i * BLOCK, BLOCK), BLOCK)],
                                     wbuf.at[slot], wsem.at[slot])

    small = [pltpu.make_async_copy(a, b, isem.at[i])
             for i, (a, b) in enumerate(((hid_hbm, hid_ref), (tok_hbm, tok_ref), (rb_hbm, rb_ref)))]
    for copy in small:
        copy.start()
    for c in range(4):
        key_copy(c).start()

    barrier = pltpu.get_barrier_semaphore()
    for p in range(1, group):
        pl.semaphore_signal(barrier, inc=1, device_id={'model': (me + p) % group}, device_id_type=MESH_ID)

    mrun[...] = jnp.full(mrun.shape, LOWEST, F32)
    srun[...] = jnp.zeros(srun.shape, F32)
    for copy in small:
        copy.wait()
    tok = tok_ref[...].astype(F32)
    gath[me, pl.ds(quarter, 8), :] = tok
    gath[me, pl.ds(extra, 8), :] = jnp.zeros((8, LANES), F32)
    gath[me, pl.ds(extra, 1), 0:rb_ref.shape[1]] = rb_ref[...].astype(F32)
    for h in range(2):
        toks[h * LANES:(h + 1) * LANES, :] = jnp.concatenate(
            [jnp.broadcast_to(tok[2 * k + h:2 * k + h + 1], (rows, LANES)) for k in range(4)], axis=0).T

    lane = lax.broadcasted_iota(jnp.int32, (quarter, LANES), 1)
    gath[me, 0:quarter, :] = jnp.zeros((quarter, LANES), F32)

    def score_step(c, carry):
        key_copy(c).wait()
        for u in range(3):
            w_copy(3 * c + u).start()
        norm = jnp.zeros((quarter, LANES), F32)
        for t in range(dim // LANES):
            x = kbuf[c, :, t * LANES:(t + 1) * LANES].astype(F32)
            norm = norm + x * x
        norm = jnp.sum(norm, axis=1, keepdims=True)
        hid4 = jnp.concatenate([hid_ref[...]] * 4, axis=0)
        dot = lax.dot_general(kbuf[c], hid4, (((1,), (1,)), ((), ())), preferred_element_type=F32)
        score = (2.0 * dot - norm) / tau_ref[0]
        score = jnp.where(lane // rows == c, score, gath[me, 0:quarter, :])
        gath[me, 0:quarter, :] = score
        return carry

    lax.fori_loop(0, 4, score_step, 0)
    for i in range(12, SLOTS):
        w_copy(i).start()

    top = functools.reduce(jnp.maximum, [gath[me, r * 8:r * 8 + 8, :] for r in range(quarter // 8)])
    top = lane_groups(jnp.broadcast_to(jnp.max(top, axis=0, keepdims=True), (8, LANES)), jnp.maximum)
    sub = lax.broadcasted_iota(jnp.int32, (8, LANES), 0)

    def run_sums(e, ids):
        for d in (1, 2, 4):
            e = e + jnp.where((ids == pltpu.roll(ids, d, 0)) & (sub >= d), pltpu.roll(e, d, 0), 0.0)
        return e

    def exp_step(r, total):
        at = [pl.ds(pl.multiple_of(r * GROUP + 8 * u, 8), 8) for u in range(2)]
        e = [jnp.exp(gath[me, a, :] - top) for a in at]
        ids = [toks[a, :] for a in at]
        sums = [run_sums(e[u], ids[u]) for u in range(2)]
        spread = lambda x: jnp.broadcast_to(x, (8, LANES))
        sums[1] = sums[1] + jnp.where(ids[1] == spread(ids[0][7:8]), spread(sums[0][7:8]), 0.0)
        after = jnp.where(sub == 7, spread(ids[1][0:1]), pltpu.roll(ids[0], 7, 0))
        gath[me, at[0], :] = jnp.where(ids[0] != after, sums[0], 0.0)
        gath[me, at[1], :] = jnp.where((ids[1] != pltpu.roll(ids[1], 7, 0)) | (sub == 7), sums[1], 0.0)
        return total + (e[0] + e[1])

    total = lax.fori_loop(0, quarter // GROUP, exp_step, jnp.zeros((8, LANES), F32), unroll=4)
    total = lane_groups(jnp.broadcast_to(jnp.sum(total, axis=0, keepdims=True), (8, LANES)), jnp.add)
    gath[me, pl.ds(extra + 1, 1), :] = top[0:1]
    gath[me, pl.ds(extra + 2, 1), :] = total[0:1]

    pl.semaphore_wait(barrier, group - 1)

    def remote(ref, slot, part, send, recv, target):
        view = ref.at[slot] if part is None else ref.at[slot, pl.ds(part * half, half)]
        return pltpu.make_async_remote_copy(view, view, send, recv, device_id={'model': target},
                                            device_id_type=MESH_ID)

    def origin(step, sign):
        return ((chip + chips + sign * step) % chips) * 2 + core

    def right_piece(s, h):
        return remote(gath, origin(s - 1, -1), h, rs.at[2 * s - 2 + h], rr.at[2 * s - 2 + h], right)

    def right_landed(s, h):
        return remote(gath, origin(s, -1), h, rs.at[2 * s - 2 + h], rr.at[2 * s - 2 + h], right)

    def left_piece(s, h):
        return remote(gath, origin(s - 1, 1), h, ls.at[2 * s - 2 + h], lr.at[2 * s - 2 + h], left)

    def left_landed(s, h):
        return remote(gath, origin(s, 1), h, ls.at[2 * s - 2 + h], lr.at[2 * s - 2 + h], left)

    def across(step, h, q):
        return remote(gath, origin(step, -1), h, ps.at[q, h], pr.at[q, h], partner)

    def across_landed(step, h, q):
        slot = origin(step, -1) + 1 - 2 * core
        return remote(gath, slot, h, ps.at[q, h], pr.at[q, h], partner)

    for h in range(2):
        right_piece(1, h).start()
        left_piece(1, h).start()
    for h in range(2):
        across(0, h, 0).start()

    right_order = [(s, h) for s in range(1, far) for h in range(2)] + [(far, 0)]
    left_order = [(s, h) for s in range(1, far) for h in range(2)] + [(far, 1)]

    def ring_event(e):
        s, h = right_order[e]
        right_landed(s, h).wait_recv()
        if (s + 1, h) in right_order:
            right_piece(s + 1, h).start()
        across(s, h, s).start()
        s, h = left_order[e]
        left_landed(s, h).wait_recv()
        if (s + 1, h) in left_order:
            left_piece(s + 1, h).start()
        across(chips - s, h, chips - s).start()

    meta_copy = pltpu.make_async_copy(meta, meta_out, osem.at[0])
    gath_copy = pltpu.make_async_copy(gath, gath_out, osem.at[1])
    scale_copy = pltpu.make_async_copy(scale_out, scale_hbm, osem.at[6])
    stat_copy_out = pltpu.make_async_copy(stat_out, stat_hbm, osem.at[7])

    def gathered():
        for q in range(chips):
            for h in range(2):
                across_landed(q, h, q).wait_recv()
        gath_copy.start()
        tile_lane = lax.broadcasted_iota(jnp.int32, (8, LANES), 1)
        place = lax.broadcasted_iota(jnp.int32, (8, LANES), 0) * LANES + tile_lane
        high = functools.reduce(jnp.maximum, [gath[g, extra + 1:extra + 2, :] for g in range(group)])
        shares = [jnp.exp(gath[g, extra + 1:extra + 2, :] - high) for g in range(group)]
        whole = sum(gath[g, extra + 2:extra + 3, :] * shares[g] for g in range(group))
        for g in range(group):
            scale_out[g:g + 1, :] = shares[g] * (lam_ref[0] / whole)

        scale_copy.start()

        def index_step(g, carry):
            bounds = gath[g, extra:extra + 8, :]
            first = jnp.sum(jnp.where(tile_lane == me, bounds, 0.0), axis=1, keepdims=True)[0:1].astype(jnp.int32)
            after = jnp.sum(jnp.where(tile_lane == me + 1, bounds, 0.0), axis=1, keepdims=True)[0:1].astype(jnp.int32)
            ids = gath[g, quarter:quarter + 8, :].astype(jnp.int32)
            meta[pl.ds(pl.multiple_of(8 * g, 8), 8), :] = jnp.where((place >= first) & (place < after),
                                                                    ids - me * width, width)
            return carry

        lax.fori_loop(0, group, index_step, 0, unroll=4)
        for g in range(group):
            meta[8 * group + g:8 * group + g + 1, :] = gath[g, extra:extra + 1, :].astype(jnp.int32)
        meta_copy.start()

    def block_stats(i, keep):
        parts = [logits[:, pl.ds(pl.multiple_of(i * BLOCK, BLOCK) + t * LANES, LANES)] for t in range(BLOCK // LANES)]
        old = mrun[...]
        new = functools.reduce(jnp.maximum, parts, old)
        srun[...] = sum((jnp.exp(x - new) for x in parts), srun[...] * jnp.exp(old - new)) * keep
        mrun[...] = new

    bands = 4
    band = width // bands

    def logit_copy(b):
        at = pl.ds(b * band, band)
        return pltpu.make_async_copy(logits.at[:, at], logit_out.at[:, at], osem.at[2 + b])

    logits[:, 0:BLOCK] = jnp.full((rows, BLOCK), LOWEST, F32)

    def w_step(i, carry):
        slot = lax.rem(i, SLOTS)
        w_copy(i).wait()
        block_stats(jnp.maximum(i - 1, 0), jnp.where(i > 0, 1.0, 0.0))
        acc = jnp.dot(hid_ref[...], wbuf[slot], preferred_element_type=F32)
        logits[:, pl.ds(pl.multiple_of(i * BLOCK, BLOCK), BLOCK)] = acc

        @pl.when(i + SLOTS < blocks)
        def _():
            w_copy(i + SLOTS).start()

        for e in range(len(right_order)):
            pl.when(i == 3 + 3 * e)(functools.partial(ring_event, e))
        pl.when(i == 4 + 3 * len(right_order))(gathered)
        for b in range(bands - 1):
            pl.when(i == (b + 1) * (blocks // bands))(logit_copy(b).start)
        return carry

    lax.fori_loop(0, blocks, w_step, 0)
    block_stats(blocks - 1, 1.0)
    logit_copy(bands - 1).start()

    peak = jnp.max(mrun[...], axis=1, keepdims=True)
    tot = jnp.sum(srun[...] * jnp.exp(mrun[...] - peak), axis=1, keepdims=True)
    pad = jnp.zeros((64 - rows, LANES), F32)
    square = jnp.concatenate([jnp.broadcast_to(peak, (rows, LANES)), pad, jnp.broadcast_to(tot, (rows, LANES)), pad],
                             axis=0)
    stats[me] = square.T[0:1]

    def stat_copy(p, slot):
        return remote(stats, slot, None, ss.at[p], sr.at[p], (me + p) % group)

    for p in range(1, group):
        stat_copy(p, me).start()
    for p in range(1, group):
        stat_copy(p, (me + group - p) % group).wait_recv()

    row_lane = lax.broadcasted_iota(jnp.int32, (1, LANES), 1)
    every = [stats[g] for g in range(group)]
    high = functools.reduce(jnp.maximum, every)
    total = jnp.zeros((1, LANES), F32)
    for one in every:
        moved = pltpu.roll(jnp.broadcast_to(one, (8, LANES)), 64, 1)[0:1]
        total = total + moved * jnp.exp(jnp.where(row_lane < rows, one - high, 0.0))
    share = (1.0 - lam_ref[0]) / jnp.where(row_lane < rows, total, 1.0)
    stat_out[0:rows] = jnp.broadcast_to(high, (LANES, LANES)).T[0:rows]
    stat_out[rows:2 * rows] = jnp.broadcast_to(share, (LANES, LANES)).T[0:rows]
    stat_copy_out.start()

    for s, h in right_order:
        right_piece(s, h).wait_send()
    for s, h in left_order:
        left_piece(s, h).wait_send()
    for q in range(chips):
        for h in range(2):
            across(q, h, q).wait_send()
    for p in range(1, group):
        stat_copy(p, me).wait_send()
    meta_copy.wait()
    gath_copy.wait()
    scale_copy.wait()
    stat_copy_out.wait()
    for b in range(bands):
        logit_copy(b).wait()


def mix_kernel(group, meta_hbm, gath_hbm, logit_hbm, scale_hbm, stat_hbm, out_hbm,
               meta, gath, logits, scale_ref, stat_ref, hist, sems, gsem, osem):
    me = lax.axis_index('model')
    rows, width = logits.shape
    span = meta.shape[0] // (group * 9) * 8
    bands = osem.shape[0]
    band = width // bands
    meta_copy = pltpu.make_async_copy(meta_hbm, meta, sems.at[0])
    logit_copy = pltpu.make_async_copy(logit_hbm, logits, sems.at[1])
    scale_copy = pltpu.make_async_copy(scale_hbm, scale_ref, sems.at[2])
    stat_copy = pltpu.make_async_copy(stat_hbm, stat_ref, sems.at[3])

    def gath_copy(g):
        return pltpu.make_async_copy(gath_hbm.at[g], gath.at[g], gsem.at[g])

    meta_copy.start()
    scale_copy.start()
    for g in range(group):
        gath_copy(g).start()
    logit_copy.start()
    stat_copy.start()

    def zero_step(i, carry):
        hist[pl.ds(pl.multiple_of(i * LANES, LANES), LANES), :] = jnp.zeros((LANES, LANES), F32)
        return carry

    lax.fori_loop(0, width // LANES, zero_step, 0)
    hist[width:width + 8, :] = jnp.zeros((8, LANES), F32)
    meta_copy.wait()
    scale_copy.wait()
    lane = lax.broadcasted_iota(jnp.int32, (1, LANES), 1)

    def source_step(g, carry):
        start = g * span
        edge = group * span + g * LANES + me
        low, high = meta[edge], meta[edge + 1]
        scale = scale_ref[pl.ds(g, 1), :]

        gath_copy(g).wait()
        begin, end = lax.shift_right_logical(low, 4), lax.shift_right_logical(high + GROUP - 1, 4)

        def table_rows(q):
            return tuple(meta[start + q * GROUP + s] for s in range(GROUP))

        def bin_step(q, at):
            factor = jnp.where(lane // rows == lax.shift_right_logical(q, 4), scale, 0.0)
            row = jnp.bitwise_and(q, 15) * GROUP
            new = [hist[pl.ds(at[s], 1), :] + gath[g, pl.ds(row + s, 1), :] * factor for s in range(GROUP)]
            for s in range(GROUP):
                hist[pl.ds(at[s], 1), :] = new[s]
            return table_rows(q + 1)

        lax.fori_loop(begin, end, bin_step, table_rows(begin))
        return carry

    lax.fori_loop(0, group, source_step, 0)
    logit_copy.wait()
    stat_copy.wait()
    peak = stat_ref[0:rows]
    share = stat_ref[rows:2 * rows]
    steps = 8

    def out_copy(b):
        at = pl.ds(pl.multiple_of(b * band, band), band)
        return pltpu.make_async_copy(logits.at[:, at], out_hbm.at[:, at], osem.at[b])

    def out_step(i, carry):
        for u in range(steps):
            at = pl.ds(pl.multiple_of(i * band + u * LANES, LANES), LANES)
            turned = hist[at, :].T
            knn = (turned[0:rows] + turned[rows:2 * rows]) + (turned[2 * rows:3 * rows] + turned[3 * rows:4 * rows])
            logits[:, at] = jnp.log(knn + jnp.exp(logits[:, at] - peak) * share)
        out_copy(i).start()
        return carry

    lax.fori_loop(0, bands, out_step, 0)
    for b in range(bands):
        out_copy(b).wait()


def solution(mesh):
    group = mesh.shape['model']

    def local_step(hidden, w_local, keys_local, tok_local, bounds_local, temperature, mix_weight):
        rows, dim = hidden.shape
        width = w_local.shape[1]
        store = keys_local.shape[0]
        quarter = store // 4
        chips = group // 2
        smem = pl.BlockSpec(memory_space=pltpu.SMEM)
        hbm = pl.BlockSpec(memory_space=pltpu.HBM)
        dma = pltpu.SemaphoreType.DMA
        gath_shape = (group, quarter + EXTRA, LANES)
        meta_shape = (group * 9, LANES)
        gath, logits, meta, scale, stat = pl.pallas_call(
            functools.partial(score_kernel, group),
            out_shape=(jax.ShapeDtypeStruct(gath_shape, F32), jax.ShapeDtypeStruct((rows, width), F32),
                       jax.ShapeDtypeStruct(meta_shape, jnp.int32), jax.ShapeDtypeStruct((group, LANES), F32),
                       jax.ShapeDtypeStruct((2 * rows, LANES), F32)),
            in_specs=[smem, smem, hbm, hbm, hbm, hbm, hbm],
            out_specs=(hbm, hbm, hbm, hbm, hbm),
            scratch_shapes=[
                pltpu.VMEM((rows, dim), jnp.bfloat16),
                pltpu.VMEM((store // LANES, LANES), jnp.int32),
                pltpu.VMEM(bounds_local.shape, jnp.int32),
                pltpu.VMEM((group, LANES), F32),
                pltpu.VMEM((2 * rows, LANES), F32),
                pltpu.VMEM((4, quarter, dim), jnp.bfloat16),
                pltpu.VMEM((SLOTS, dim, BLOCK), jnp.bfloat16),
                pltpu.VMEM(gath_shape, F32),
                pltpu.VMEM((rows, width), F32),
                pltpu.VMEM((quarter, LANES), F32),
                pltpu.VMEM(meta_shape, jnp.int32),
                pltpu.VMEM((rows, LANES), F32),
                pltpu.VMEM((rows, LANES), F32),
                pltpu.VMEM((group, 1, LANES), F32),
                dma((3,)), dma((4,)), dma((SLOTS,)), dma((8,)),
                dma((chips,)), dma((chips,)), dma((chips,)), dma((chips,)),
                dma((chips, 2)), dma((chips, 2)),
                dma((group,)), dma((group,)),
            ],
            compiler_params=pltpu.CompilerParams(collective_id=0, has_side_effects=True, vmem_limit_bytes=VMEM_BYTES),
            name='score_gather_head',
        )(temperature.reshape(1), mix_weight.reshape(1), hidden, tok_local.reshape(store // LANES, LANES), bounds_local,
          keys_local, w_local)
        return mix_call(group, rows, width, meta, gath, logits, scale, stat)

    return jax.shard_map(local_step, mesh=mesh,
                         in_specs=(P('data', None), P(None, 'model'), P('model', None), P('model'),
                                   P('model', None), P(), P()),
                         out_specs=P('data', 'model'), check_vma=False)


def mix_call(group, rows, width, meta, gath, logits, scale, stat):
    hbm = pl.BlockSpec(memory_space=pltpu.HBM)
    dma = pltpu.SemaphoreType.DMA
    return pl.pallas_call(
        functools.partial(mix_kernel, group),
        out_shape=jax.ShapeDtypeStruct((rows, width), F32),
        in_specs=[hbm] * 5,
        out_specs=hbm,
        scratch_shapes=[
            pltpu.SMEM((meta.size,), jnp.int32),
            pltpu.VMEM(gath.shape, F32),
            pltpu.VMEM((rows, width), F32),
            pltpu.VMEM(scale.shape, F32),
            pltpu.VMEM(stat.shape, F32),
            pltpu.VMEM((width + 8, LANES), F32),
            dma((4,)), dma((group,)), dma((width // (8 * LANES),)),
        ],
        compiler_params=pltpu.CompilerParams(vmem_limit_bytes=VMEM_BYTES),
        name='bin_mix',
    )(meta.reshape(meta.size), gath, logits, scale, stat)
```

```python
import functools

import jax
import jax.numpy as jnp
from jax import lax
from jax.experimental import pallas as pl
from jax.experimental.pallas import tpu as pltpu
from jax.sharding import PartitionSpec as P

MESH_ID = pl.DeviceIdType.MESH
LANES = 128
BLOCK = 256
SLOTS = 14
GROUP = 16
F32 = jnp.float32
LOWEST = float(jnp.finfo(jnp.float32).min)
VMEM_BYTES = 64 * 1024 * 1024 - 65536
EXTRA = 16


def lane_groups(x, op):
    x = op(x, pltpu.roll(x, 64, 1))
    return op(x, pltpu.roll(x, 32, 1))


def score_kernel(group, tau_ref, lam_ref, hid_hbm, tok_hbm, rb_hbm, keys_ref, w_ref,
                 gath_out, logit_out, meta_out, scale_hbm, stat_hbm,
                 hid_ref, tok_ref, rb_ref, scale_out, stat_out, kbuf, wbuf, gath, logits, toks, meta, mrun, srun, stats,
                 isem, ksem, wsem, osem, rs, rr, ls, lr, ps, pr, ss, sr):
    me = lax.axis_index('model')
    chips = group // 2
    chip, core = me // 2, me % 2
    partner = me + 1 - 2 * core
    right = ((chip + 1) % chips) * 2 + core
    left = ((chip + chips - 1) % chips) * 2 + core
    rows, dim = hid_ref.shape
    quarter = kbuf.shape[1]
    half = (quarter + EXTRA) // 2
    width = logits.shape[1]
    blocks = width // BLOCK
    far = chips // 2
    extra = quarter + 8

    def key_copy(c):
        return pltpu.make_async_copy(keys_ref.at[pl.ds(pl.multiple_of(c * quarter, quarter), quarter)],
                                     kbuf.at[c], ksem.at[c])

    def w_copy(i):
        slot = lax.rem(i, SLOTS)
        return pltpu.make_async_copy(w_ref.at[:, pl.ds(pl.multiple_of(i * BLOCK, BLOCK), BLOCK)],
                                     wbuf.at[slot], wsem.at[slot])

    small = [pltpu.make_async_copy(a, b, isem.at[i])
             for i, (a, b) in enumerate(((hid_hbm, hid_ref), (tok_hbm, tok_ref), (rb_hbm, rb_ref)))]
    for copy in small:
        copy.start()
    for c in range(4):
        key_copy(c).start()

    barrier = pltpu.get_barrier_semaphore()
    for p in range(1, group):
        pl.semaphore_signal(barrier, inc=1, device_id={'model': (me + p) % group}, device_id_type=MESH_ID)

    mrun[...] = jnp.full(mrun.shape, LOWEST, F32)
    srun[...] = jnp.zeros(srun.shape, F32)
    for copy in small:
        copy.wait()
    tok = tok_ref[...].astype(F32)
    gath[me, pl.ds(quarter, 8), :] = tok
    gath[me, pl.ds(extra, 8), :] = jnp.zeros((8, LANES), F32)
    gath[me, pl.ds(extra, 1), 0:rb_ref.shape[1]] = rb_ref[...].astype(F32)
    for h in range(2):
        toks[h * LANES:(h + 1) * LANES, :] = jnp.concatenate(
            [jnp.broadcast_to(tok[2 * k + h:2 * k + h + 1], (rows, LANES)) for k in range(4)], axis=0).T

    lane = lax.broadcasted_iota(jnp.int32, (quarter, LANES), 1)
    gath[me, 0:quarter, :] = jnp.zeros((quarter, LANES), F32)

    def score_step(c, carry):
        key_copy(c).wait()
        for u in range(3):
            w_copy(3 * c + u).start()
        norm = jnp.zeros((quarter, LANES), F32)
        for t in range(dim // LANES):
            x = kbuf[c, :, t * LANES:(t + 1) * LANES].astype(F32)
            norm = norm + x * x
        norm = jnp.sum(norm, axis=1, keepdims=True)
        hid4 = jnp.concatenate([hid_ref[...]] * 4, axis=0)
        dot = lax.dot_general(kbuf[c], hid4, (((1,), (1,)), ((), ())), preferred_element_type=F32)
        score = (2.0 * dot - norm) / tau_ref[0]
        score = jnp.where(lane // rows == c, score, gath[me, 0:quarter, :])
        gath[me, 0:quarter, :] = score
        return carry

    lax.fori_loop(0, 4, score_step, 0)
    for i in range(12, SLOTS):
        w_copy(i).start()

    top = functools.reduce(jnp.maximum, [gath[me, r * 8:r * 8 + 8, :] for r in range(quarter // 8)])
    top = lane_groups(jnp.broadcast_to(jnp.max(top, axis=0, keepdims=True), (8, LANES)), jnp.maximum)
    sub = lax.broadcasted_iota(jnp.int32, (8, LANES), 0)

    def run_sums(e, ids):
        for d in (1, 2, 4):
            e = e + jnp.where((ids == pltpu.roll(ids, d, 0)) & (sub >= d), pltpu.roll(e, d, 0), 0.0)
        return e

    def exp_step(r, total):
        at = [pl.ds(pl.multiple_of(r * GROUP + 8 * u, 8), 8) for u in range(2)]
        e = [jnp.exp(gath[me, a, :] - top) for a in at]
        ids = [toks[a, :] for a in at]
        sums = [run_sums(e[u], ids[u]) for u in range(2)]
        spread = lambda x: jnp.broadcast_to(x, (8, LANES))
        sums[1] = sums[1] + jnp.where(ids[1] == spread(ids[0][7:8]), spread(sums[0][7:8]), 0.0)
        after = jnp.where(sub == 7, spread(ids[1][0:1]), pltpu.roll(ids[0], 7, 0))
        gath[me, at[0], :] = jnp.where(ids[0] != after, sums[0], 0.0)
        gath[me, at[1], :] = jnp.where((ids[1] != pltpu.roll(ids[1], 7, 0)) | (sub == 7), sums[1], 0.0)
        return total + (e[0] + e[1])

    total = lax.fori_loop(0, quarter // GROUP, exp_step, jnp.zeros((8, LANES), F32), unroll=4)
    total = lane_groups(jnp.broadcast_to(jnp.sum(total, axis=0, keepdims=True), (8, LANES)), jnp.add)
    gath[me, pl.ds(extra + 1, 1), :] = top[0:1]
    gath[me, pl.ds(extra + 2, 1), :] = total[0:1]

    pl.semaphore_wait(barrier, group - 1)

    def remote(ref, slot, part, send, recv, target):
        view = ref.at[slot] if part is None else ref.at[slot, pl.ds(part * half, half)]
        return pltpu.make_async_remote_copy(view, view, send, recv, device_id={'model': target},
                                            device_id_type=MESH_ID)

    def origin(step, sign):
        return ((chip + chips + sign * step) % chips) * 2 + core

    def right_piece(s, h):
        return remote(gath, origin(s - 1, -1), h, rs.at[2 * s - 2 + h], rr.at[2 * s - 2 + h], right)

    def right_landed(s, h):
        return remote(gath, origin(s, -1), h, rs.at[2 * s - 2 + h], rr.at[2 * s - 2 + h], right)

    def left_piece(s, h):
        return remote(gath, origin(s - 1, 1), h, ls.at[2 * s - 2 + h], lr.at[2 * s - 2 + h], left)

    def left_landed(s, h):
        return remote(gath, origin(s, 1), h, ls.at[2 * s - 2 + h], lr.at[2 * s - 2 + h], left)

    def across(step, h, q):
        return remote(gath, origin(step, -1), h, ps.at[q, h], pr.at[q, h], partner)

    def across_landed(step, h, q):
        slot = origin(step, -1) + 1 - 2 * core
        return remote(gath, slot, h, ps.at[q, h], pr.at[q, h], partner)

    for h in range(2):
        right_piece(1, h).start()
        left_piece(1, h).start()
    for h in range(2):
        across(0, h, 0).start()

    right_order = [(s, h) for s in range(1, far) for h in range(2)] + [(far, 0)]
    left_order = [(s, h) for s in range(1, far) for h in range(2)] + [(far, 1)]

    def ring_event(e):
        s, h = right_order[e]
        right_landed(s, h).wait_recv()
        if (s + 1, h) in right_order:
            right_piece(s + 1, h).start()
        across(s, h, s).start()
        s, h = left_order[e]
        left_landed(s, h).wait_recv()
        if (s + 1, h) in left_order:
            left_piece(s + 1, h).start()
        across(chips - s, h, chips - s).start()

    meta_copy = pltpu.make_async_copy(meta, meta_out, osem.at[0])
    gath_copy = pltpu.make_async_copy(gath, gath_out, osem.at[1])
    scale_copy = pltpu.make_async_copy(scale_out, scale_hbm, osem.at[6])
    stat_copy_out = pltpu.make_async_copy(stat_out, stat_hbm, osem.at[7])

    def gathered():
        for q in range(chips):
            for h in range(2):
                across_landed(q, h, q).wait_recv()
        gath_copy.start()
        tile_lane = lax.broadcasted_iota(jnp.int32, (8, LANES), 1)
        place = lax.broadcasted_iota(jnp.int32, (8, LANES), 0) * LANES + tile_lane
        high = functools.reduce(jnp.maximum, [gath[g, extra + 1:extra + 2, :] for g in range(group)])
        shares = [jnp.exp(gath[g, extra + 1:extra + 2, :] - high) for g in range(group)]
        whole = sum(gath[g, extra + 2:extra + 3, :] * shares[g] for g in range(group))
        for g in range(group):
            scale_out[g:g + 1, :] = shares[g] * (lam_ref[0] / whole)

        scale_copy.start()

        def index_step(g, carry):
            bounds = gath[g, extra:extra + 8, :]
            first = jnp.sum(jnp.where(tile_lane == me, bounds, 0.0), axis=1, keepdims=True)[0:1].astype(jnp.int32)
            after = jnp.sum(jnp.where(tile_lane == me + 1, bounds, 0.0), axis=1, keepdims=True)[0:1].astype(jnp.int32)
            ids = gath[g, quarter:quarter + 8, :].astype(jnp.int32)
            meta[pl.ds(pl.multiple_of(8 * g, 8), 8), :] = jnp.where((place >= first) & (place < after),
                                                                    ids - me * width, width)
            return carry

        lax.fori_loop(0, group, index_step, 0, unroll=4)
        for g in range(group):
            meta[8 * group + g:8 * group + g + 1, :] = gath[g, extra:extra + 1, :].astype(jnp.int32)
        meta_copy.start()

    def block_stats(i, keep):
        parts = [logits[:, pl.ds(pl.multiple_of(i * BLOCK, BLOCK) + t * LANES, LANES)] for t in range(BLOCK // LANES)]
        old = mrun[...]
        new = functools.reduce(jnp.maximum, parts, old)
        srun[...] = sum((jnp.exp(x - new) for x in parts), srun[...] * jnp.exp(old - new)) * keep
        mrun[...] = new

    bands = 4
    band = width // bands

    def logit_copy(b):
        at = pl.ds(b * band, band)
        return pltpu.make_async_copy(logits.at[:, at], logit_out.at[:, at], osem.at[2 + b])

    logits[:, 0:BLOCK] = jnp.full((rows, BLOCK), LOWEST, F32)

    def w_step(i, carry):
        slot = lax.rem(i, SLOTS)
        w_copy(i).wait()
        block_stats(jnp.maximum(i - 1, 0), jnp.where(i > 0, 1.0, 0.0))
        acc = jnp.dot(hid_ref[...], wbuf[slot], preferred_element_type=F32)
        logits[:, pl.ds(pl.multiple_of(i * BLOCK, BLOCK), BLOCK)] = acc

        @pl.when(i + SLOTS < blocks)
        def _():
            w_copy(i + SLOTS).start()

        for e in range(len(right_order)):
            pl.when(i == 6 + 3 * e)(functools.partial(ring_event, e))
        pl.when(i == 7 + 3 * len(right_order))(gathered)
        for b in range(bands - 1):
            pl.when(i == (b + 1) * (blocks // bands))(logit_copy(b).start)
        return carry

    lax.fori_loop(0, blocks, w_step, 0)
    block_stats(blocks - 1, 1.0)
    logit_copy(bands - 1).start()

    peak = jnp.max(mrun[...], axis=1, keepdims=True)
    tot = jnp.sum(srun[...] * jnp.exp(mrun[...] - peak), axis=1, keepdims=True)
    pad = jnp.zeros((64 - rows, LANES), F32)
    square = jnp.concatenate([jnp.broadcast_to(peak, (rows, LANES)), pad, jnp.broadcast_to(tot, (rows, LANES)), pad],
                             axis=0)
    stats[me] = square.T[0:1]

    def stat_copy(p, slot):
        return remote(stats, slot, None, ss.at[p], sr.at[p], (me + p) % group)

    for p in range(1, group):
        stat_copy(p, me).start()
    for p in range(1, group):
        stat_copy(p, (me + group - p) % group).wait_recv()

    row_lane = lax.broadcasted_iota(jnp.int32, (1, LANES), 1)
    every = [stats[g] for g in range(group)]
    high = functools.reduce(jnp.maximum, every)
    total = jnp.zeros((1, LANES), F32)
    for one in every:
        moved = pltpu.roll(jnp.broadcast_to(one, (8, LANES)), 64, 1)[0:1]
        total = total + moved * jnp.exp(jnp.where(row_lane < rows, one - high, 0.0))
    share = (1.0 - lam_ref[0]) / jnp.where(row_lane < rows, total, 1.0)
    stat_out[0:rows] = jnp.broadcast_to(high, (LANES, LANES)).T[0:rows]
    stat_out[rows:2 * rows] = jnp.broadcast_to(share, (LANES, LANES)).T[0:rows]
    stat_copy_out.start()

    for s, h in right_order:
        right_piece(s, h).wait_send()
    for s, h in left_order:
        left_piece(s, h).wait_send()
    for q in range(chips):
        for h in range(2):
            across(q, h, q).wait_send()
    for p in range(1, group):
        stat_copy(p, me).wait_send()
    meta_copy.wait()
    gath_copy.wait()
    scale_copy.wait()
    stat_copy_out.wait()
    for b in range(bands):
        logit_copy(b).wait()


def mix_kernel(group, meta_hbm, gath_hbm, logit_hbm, scale_hbm, stat_hbm, out_hbm,
               meta, gath, logits, scale_ref, stat_ref, hist, sems, gsem, osem):
    me = lax.axis_index('model')
    rows, width = logits.shape
    span = meta.shape[0] // (group * 9) * 8
    bands = osem.shape[0]
    band = width // bands
    meta_copy = pltpu.make_async_copy(meta_hbm, meta, sems.at[0])
    logit_copy = pltpu.make_async_copy(logit_hbm, logits, sems.at[1])
    scale_copy = pltpu.make_async_copy(scale_hbm, scale_ref, sems.at[2])
    stat_copy = pltpu.make_async_copy(stat_hbm, stat_ref, sems.at[3])

    def gath_copy(g):
        return pltpu.make_async_copy(gath_hbm.at[g], gath.at[g], gsem.at[g])

    meta_copy.start()
    scale_copy.start()
    for g in range(group):
        gath_copy(g).start()
    logit_copy.start()
    stat_copy.start()

    def zero_step(i, carry):
        hist[pl.ds(pl.multiple_of(i * LANES, LANES), LANES), :] = jnp.zeros((LANES, LANES), F32)
        return carry

    lax.fori_loop(0, width // LANES, zero_step, 0)
    hist[width:width + 8, :] = jnp.zeros((8, LANES), F32)
    meta_copy.wait()
    scale_copy.wait()
    lane = lax.broadcasted_iota(jnp.int32, (1, LANES), 1)

    def source_step(g, carry):
        start = g * span
        edge = group * span + g * LANES + me
        low, high = meta[edge], meta[edge + 1]
        scale = scale_ref[pl.ds(g, 1), :]

        gath_copy(g).wait()
        begin, end = lax.shift_right_logical(low, 4), lax.shift_right_logical(high + GROUP - 1, 4)

        def table_rows(q):
            return tuple(meta[start + q * GROUP + s] for s in range(GROUP))

        def bin_step(q, at):
            factor = jnp.where(lane // rows == lax.shift_right_logical(q, 4), scale, 0.0)
            row = jnp.bitwise_and(q, 15) * GROUP
            new = [hist[pl.ds(at[s], 1), :] + gath[g, pl.ds(row + s, 1), :] * factor for s in range(GROUP)]
            for s in range(GROUP):
                hist[pl.ds(at[s], 1), :] = new[s]
            return table_rows(q + 1)

        lax.fori_loop(begin, end, bin_step, table_rows(begin))
        return carry

    lax.fori_loop(0, group, source_step, 0)
    logit_copy.wait()
    stat_copy.wait()
    peak = stat_ref[0:rows]
    share = stat_ref[rows:2 * rows]
    steps = band // LANES

    def out_copy(b):
        at = pl.ds(pl.multiple_of(b * band, band), band)
        return pltpu.make_async_copy(logits.at[:, at], out_hbm.at[:, at], osem.at[b])

    def out_step(i, carry):
        for u in range(steps):
            at = pl.ds(pl.multiple_of(i * band + u * LANES, LANES), LANES)
            turned = hist[at, :].T
            knn = (turned[0:rows] + turned[rows:2 * rows]) + (turned[2 * rows:3 * rows] + turned[3 * rows:4 * rows])
            logits[:, at] = jnp.log(knn + jnp.exp(logits[:, at] - peak) * share)
        out_copy(i).start()
        return carry

    lax.fori_loop(0, bands, out_step, 0)
    for b in range(bands):
        out_copy(b).wait()


def solution(mesh):
    group = mesh.shape['model']

    def local_step(hidden, w_local, keys_local, tok_local, bounds_local, temperature, mix_weight):
        rows, dim = hidden.shape
        width = w_local.shape[1]
        store = keys_local.shape[0]
        quarter = store // 4
        chips = group // 2
        smem = pl.BlockSpec(memory_space=pltpu.SMEM)
        hbm = pl.BlockSpec(memory_space=pltpu.HBM)
        dma = pltpu.SemaphoreType.DMA
        gath_shape = (group, quarter + EXTRA, LANES)
        meta_shape = (group * 9, LANES)
        gath, logits, meta, scale, stat = pl.pallas_call(
            functools.partial(score_kernel, group),
            out_shape=(jax.ShapeDtypeStruct(gath_shape, F32), jax.ShapeDtypeStruct((rows, width), F32),
                       jax.ShapeDtypeStruct(meta_shape, jnp.int32), jax.ShapeDtypeStruct((group, LANES), F32),
                       jax.ShapeDtypeStruct((2 * rows, LANES), F32)),
            in_specs=[smem, smem, hbm, hbm, hbm, hbm, hbm],
            out_specs=(hbm, hbm, hbm, hbm, hbm),
            scratch_shapes=[
                pltpu.VMEM((rows, dim), jnp.bfloat16),
                pltpu.VMEM((store // LANES, LANES), jnp.int32),
                pltpu.VMEM(bounds_local.shape, jnp.int32),
                pltpu.VMEM((group, LANES), F32),
                pltpu.VMEM((2 * rows, LANES), F32),
                pltpu.VMEM((4, quarter, dim), jnp.bfloat16),
                pltpu.VMEM((SLOTS, dim, BLOCK), jnp.bfloat16),
                pltpu.VMEM(gath_shape, F32),
                pltpu.VMEM((rows, width), F32),
                pltpu.VMEM((quarter, LANES), F32),
                pltpu.VMEM(meta_shape, jnp.int32),
                pltpu.VMEM((rows, LANES), F32),
                pltpu.VMEM((rows, LANES), F32),
                pltpu.VMEM((group, 1, LANES), F32),
                dma((3,)), dma((4,)), dma((SLOTS,)), dma((8,)),
                dma((chips,)), dma((chips,)), dma((chips,)), dma((chips,)),
                dma((chips, 2)), dma((chips, 2)),
                dma((group,)), dma((group,)),
            ],
            compiler_params=pltpu.CompilerParams(collective_id=0, has_side_effects=True, vmem_limit_bytes=VMEM_BYTES),
            name='score_gather_head',
        )(temperature.reshape(1), mix_weight.reshape(1), hidden, tok_local.reshape(store // LANES, LANES), bounds_local,
          keys_local, w_local)
        return mix_call(group, rows, width, meta, gath, logits, scale, stat)

    return jax.shard_map(local_step, mesh=mesh,
                         in_specs=(P('data', None), P(None, 'model'), P('model', None), P('model'),
                                   P('model', None), P(), P()),
                         out_specs=P('data', 'model'), check_vma=False)


def mix_call(group, rows, width, meta, gath, logits, scale, stat):
    hbm = pl.BlockSpec(memory_space=pltpu.HBM)
    dma = pltpu.SemaphoreType.DMA
    return pl.pallas_call(
        functools.partial(mix_kernel, group),
        out_shape=jax.ShapeDtypeStruct((rows, width), F32),
        in_specs=[hbm] * 5,
        out_specs=hbm,
        scratch_shapes=[
            pltpu.SMEM((meta.size,), jnp.int32),
            pltpu.VMEM(gath.shape, F32),
            pltpu.VMEM((rows, width), F32),
            pltpu.VMEM(scale.shape, F32),
            pltpu.VMEM(stat.shape, F32),
            pltpu.VMEM((width + 8, LANES), F32),
            dma((4,)), dma((group,)), dma((width // (16 * LANES),)),
        ],
        compiler_params=pltpu.CompilerParams(vmem_limit_bytes=VMEM_BYTES),
        name='bin_mix',
    )(meta.reshape(meta.size), gath, logits, scale, stat)
```
